512 devices in a mesh: row: 32 (over y, x), col: 16 (over z, core).
Axes of the slice: x: 4, y: 8, z: 8, core: 2. Of those that a mesh axis runs over, the one named last changes fastest.
Arguments:
- relu21_preact: bfloat16 [1024, 1024, 128], P('row', 'col'), may hold values from -6 to 6
- relu22_preact: bfloat16 [1024, 1024, 128], P('row', 'col'), may hold values from -600 to 600
- relu31_preact: bfloat16 [512, 512, 256], P('row', 'col'), may hold values from -6 to 6
- relu32_preact: bfloat16 [512, 512, 256], P('row', 'col'), may hold values from -6 to 6
- relu33_preact: bfloat16 [512, 512, 256], P('row', 'col'), may hold values from -600 to 600
- target22_preact: bfloat16 [1024, 1024, 128], P('row', 'col'), may hold values from -600 to 600
- target33_preact: bfloat16 [512, 512, 256], P('row', 'col'), may hold values from -600 to 600
- pool1_argmax: int32 [1024, 65536], P('row', 'col'), may hold values from 0 to 3
- pool2_argmax: int32 [512, 65536], P('row', 'col'), may hold values from 0 to 3
- linear2_weight: float32 [128], replicated, may hold values from 0.2 to 2
- linear3_weight: float32 [256], replicated, may hold values from 0.2 to 2
- kernel21: bfloat16 [128, 576], replicated, may hold values from -0.25 to 0.25
- kernel22: bfloat16 [128, 1152], replicated, may hold values from -0.1875 to 0.1875
- kernel31: bfloat16 [256, 1152], replicated, may hold values from -0.1875 to 0.1875
- kernel32: bfloat16 [256, 2304], replicated, may hold values from -0.125 to 0.125
- kernel33: bfloat16 [256, 2304], replicated, may hold values from -0.125 to 0.125
Outputs:
- relu12_gradient: bfloat16 [2048, 131072], P('row', 'col')
The draws below stay inside these ranges and needn't reach their ends.
Inputs may be any that keep to these rules, and one draw needn't show every extreme that they name: `pool1_argmax`: the position of the maximum in each 2x2 window, 0 top left, 1 top right, 2 bottom left, 3 bottom right; entry [r, c * 64 + ch] belongs to pooled cell (r, c) and channel ch. `pool2_argmax`: as for pool1_argmax, with 128 channels.
All inputs are finite; a program needn't handle non-finite values.
Results may differ from the reference program's by a relative error of at most 0.0059.
Values may be sent and summed in bfloat16 or wider, within the bound.
No kernel may reach another device: no remote copies, remote signals or barrier semaphores. Data moves between devices by JAX's collectives and lax.ppermute only.
A program may use at most 64 MiB of HBM per device.

```python
import math
import jax
import jax.numpy as jnp
from jax import lax

CH1 = 64
CH2 = 128
CH3 = 256
HEIGHT = 512
WIDTH = 512


def tap_values(key, salt, height, breadth, channels):
    folded = jax.random.fold_in(key, salt)
    streams = jax.random.split(folded, 3)
    spread = math.log(10.0)
    values = jnp.clip(jax.random.normal(streams[2], (height, breadth, channels), jnp.float32), -4.0, 4.0)
    channel_scale = jnp.exp(jax.random.uniform(streams[0], (channels,), jnp.float32, 0.0, spread))
    pixel_scale = jnp.exp(jax.random.uniform(streams[1], (height, breadth, 1), jnp.float32, 0.0, spread))
    return (values * channel_scale * pixel_scale).astype(jnp.bfloat16)


def draw_relu22_preact(key, part):
    return tap_values(key, 11, 2 * HEIGHT, 2 * WIDTH, CH2)


def draw_relu33_preact(key, part):
    return tap_values(key, 12, HEIGHT, WIDTH, CH3)


def draw_target22_preact(key, part):
    return tap_values(key, 13, 2 * HEIGHT, 2 * WIDTH, CH2)


def draw_target33_preact(key, part):
    return tap_values(key, 14, HEIGHT, WIDTH, CH3)


def plant(drawn, own_key, least, top_value):
    index_at = [jax.random.randint(jax.random.fold_in(own_key, axis), (), 0, length) for axis, length in enumerate(drawn.shape)]
    longest = drawn.shape.index(max(drawn.shape))
    next_to = index_at[:longest] + [(index_at[longest] + 1) % drawn.shape[longest]] + index_at[longest + 1:]
    return drawn.at[tuple(index_at)].set(least).at[tuple(next_to)].set(top_value)


def levels(stream_key, dims, cuts, smallest, high):
    def one(dim, shards_of):
        draws = jax.random.uniform(jax.random.fold_in(jax.random.fold_in(stream_key, 6), dim), (shards_of,), jnp.float32, smallest / len(cuts), high / len(cuts))
        return jnp.repeat(jnp.exp(draws), dims[dim] // shards_of).reshape((-1,) + (1,) * (len(dims) - dim - 1))

    gain = one(*cuts[0])
    for cut in cuts[1:]:
        gain = gain * one(*cut)
    return gain


def centred(rng, shape, scale, limit, cuts=(), held_as=jnp.bfloat16):
    entries = scale * jax.random.normal(rng, shape, jnp.float32)
    if cuts:
        entries = entries * levels(rng, shape, cuts, -0.22, 0.18)
    return jnp.clip(entries, -limit, limit).astype(held_as)


def setup_inputs(seed: int = 0) -> dict:
    splits = jax.random.split(jax.random.key(seed), 17)
    return {
        "relu21_preact": centred(splits[0], (2 * HEIGHT, 2 * WIDTH, CH2), 1.0, 6.0, ((0, 32), (1, 16))),
        "relu22_preact": draw_relu22_preact(jax.random.fold_in(splits[16], 71), 0),
        "relu31_preact": centred(splits[2], (HEIGHT, WIDTH, CH3), 1.0, 6.0, ((0, 32), (1, 16))),
        "relu32_preact": centred(splits[3], (HEIGHT, WIDTH, CH3), 1.0, 6.0, ((0, 32), (1, 16))),
        "relu33_preact": draw_relu33_preact(jax.random.fold_in(splits[16], 71), 0),
        "target22_preact": draw_target22_preact(jax.random.fold_in(splits[16], 71), 0),
        "target33_preact": draw_target33_preact(jax.random.fold_in(splits[16], 71), 0),
        "pool1_argmax": plant(jax.random.randint(splits[7], (2 * HEIGHT, 2 * WIDTH * CH1), 0, 4), jax.random.fold_in(splits[7], 1), 0, 3).astype(jnp.int32),
        "pool2_argmax": plant(jax.random.randint(splits[8], (HEIGHT, WIDTH * CH2), 0, 4), jax.random.fold_in(splits[8], 1), 0, 3).astype(jnp.int32),
        "linear2_weight": jnp.clip(jnp.exp(jax.random.uniform(splits[9], (CH2,), jnp.float32, math.log(0.2), math.log(2.0))), 0.2, 2.0),
        "linear3_weight": jnp.clip(jnp.exp(jax.random.uniform(splits[10], (CH3,), jnp.float32, math.log(0.2), math.log(2.0))), 0.2, 2.0),
        "kernel21": centred(splits[11], (CH2, 9 * CH1), (9 * CH1) ** -0.5, 0.25),
        "kernel22": centred(splits[12], (CH2, 9 * CH2), (9 * CH2) ** -0.5, 0.1875),
        "kernel31": centred(splits[13], (CH3, 9 * CH2), (9 * CH2) ** -0.5, 0.1875),
        "kernel32": centred(splits[14], (CH3, 9 * CH3), (9 * CH3) ** -0.5, 0.125),
        "kernel33": centred(splits[15], (CH3, 9 * CH3), (9 * CH3) ** -0.5, 0.125),
    }


EPSILON = 1e-06

def inject(preact, target, weight):
    feature = jnp.maximum(preact.astype(jnp.float32), 0.0)
    wanted = jnp.maximum(target.astype(jnp.float32), 0.0)
    feature_norm = jnp.sqrt(lax.optimization_barrier(jnp.mean(feature * feature, axis=-1, keepdims=True)) + EPSILON)
    wanted_norm = jnp.sqrt(lax.optimization_barrier(jnp.mean(wanted * wanted, axis=-1, keepdims=True)) + EPSILON)
    scaled = feature / feature_norm
    excess = 2.0 * weight * (scaled - wanted / wanted_norm)
    return (excess - scaled * lax.optimization_barrier(jnp.mean(excess * scaled, axis=-1, keepdims=True))) / feature_norm

def masked(preact, values):
    return jnp.where(preact > 0, values, 0.0).astype(jnp.bfloat16)

def unpool(values, argmax_rows):
    height, breadth, channels = values.shape
    position = argmax_rows.reshape(height, breadth, channels)
    stripes = []
    for vertical in range(2):
        halves = [jnp.where(position == 2 * vertical + lateral, values, 0.0) for lateral in range(2)]
        stripes.append(jnp.stack(halves, axis=2))
    return jnp.stack(stripes, axis=1).reshape(2 * height, 2 * breadth, channels)

def back_conv(gradient, kernel):
    outputs = kernel.shape[0]
    channels_in = kernel.shape[1] // 9
    flipped = kernel.reshape(outputs, 3, 3, channels_in)[:, ::-1, ::-1, :]
    flipped = flipped.transpose(1, 2, 0, 3).astype(jnp.float32)
    result = lax.conv_general_dilated(gradient.astype(jnp.float32)[None], flipped, (1, 1), 'SAME', dimension_numbers=('NHWC', 'HWIO', 'NHWC'), precision=lax.Precision.HIGHEST)
    return result[0]

def reference(relu21_preact, relu22_preact, relu31_preact, relu32_preact, relu33_preact, target22_preact, target33_preact, pool1_argmax, pool2_argmax, linear2_weight, linear3_weight, kernel21, kernel22, kernel31, kernel32, kernel33):
    seeded = masked(relu33_preact, inject(relu33_preact, target33_preact, linear3_weight))
    gradient32 = masked(relu32_preact, back_conv(seeded, kernel33))
    gradient31 = masked(relu31_preact, back_conv(gradient32, kernel32))
    pooled2 = back_conv(gradient31, kernel31)
    arriving = unpool(pooled2, pool2_argmax) + inject(relu22_preact, target22_preact, linear2_weight)
    gradient22 = masked(relu22_preact, arriving)
    gradient21 = masked(relu21_preact, back_conv(gradient22, kernel22))
    pooled1 = back_conv(gradient21, kernel21)
    result = unpool(pooled1, pool1_argmax).astype(jnp.bfloat16)
    return result.reshape(result.shape[0], -1)
```

```python
import jax
import jax.numpy as jnp
from jax import lax
from jax.experimental import pallas as pl
from jax.experimental.pallas import tpu as pltpu
from jax.sharding import PartitionSpec as P

EPSILON = 1e-06
F32 = jnp.float32
BF16 = jnp.bfloat16

ROW_SEED, ROW_M32, ROW_M31, ROW_M22, ROW_I22, ROW_M21, ROW_A2, ROW_TOTAL = (
    0, 256, 448, 576, 704, 832, 896, 928)
COL_SEED, COL_M32, COL_M31, COL_M22, COL_I22, COL_M21, COL_A2, COL_TOTAL = (
    0, 192, 336, 432, 512, 592, 632, 656)
W3 = 48
W2 = 80
WU = 96
WP = 88
LEAD = 8


def inject(preact, target, weight):
    count = preact.shape[-1]
    feature = jnp.maximum(preact.astype(F32), 0.0)
    wanted = jnp.maximum(target.astype(F32), 0.0)
    scale = lax.rsqrt(jnp.sum(feature * feature, axis=-1, keepdims=True) * (1.0 / count) + EPSILON)
    other = lax.rsqrt(jnp.sum(wanted * wanted, axis=-1, keepdims=True) * (1.0 / count) + EPSILON)
    scaled = feature * scale
    excess = (2.0 * weight) * (scaled - wanted * other)
    mean = jnp.sum(excess * scaled, axis=-1, keepdims=True) * (1.0 / count)
    return (excess - scaled * mean) * scale


def pack_rows(m33, t33, m32, m31, m22t, m22b, t22t, t22b, m21t, m21b, a2, w2, w3, seeds, up, down):
    rows, cols, ch = m33.shape
    step = 4
    for r in range(0, rows, step):
        p = m33[r : r + step].reshape(step * cols, ch)
        value = inject(p, t33[r : r + step].reshape(step * cols, ch), w3[...])
        value = jnp.where(p.astype(F32) > 0, value, 0.0).astype(BF16)
        seeds[r : r + step] = value.reshape(step, cols, ch)
    for out, first, m22, t22, m21, edge in (
        (up, 0, m22t, t22t, m21t, 0),
        (down, 1, m22b, t22b, m21b, rows - 1),
    ):
        for source, base, width in ((seeds, ROW_SEED, 4), (m32, ROW_M32, 3), (m31, ROW_M31, 2)):
            begin = rows - width if first else 0
            for k in range(width):
                for h in range(2):
                    at = base + (k * 2 + h) * cols
                    out[at : at + cols] = source[begin + k, :, h * 128 : (h + 1) * 128]
        wide = m22.shape[1]
        p = m22[...].reshape(2 * wide, 128)
        out[ROW_M22 : ROW_M22 + 2 * wide] = p
        out[ROW_I22 : ROW_I22 + 2 * wide] = inject(
            p, t22[...].reshape(2 * wide, 128), w2[...]
        ).astype(BF16)
        out[ROW_M21 : ROW_M21 + wide] = m21[0]
        line = a2[edge : edge + 1, :].astype(F32)
        line = jnp.concatenate([line[:, c * 128 : (c + 1) * 128] for c in range(cols)], axis=0)
        out[ROW_A2 : ROW_A2 + cols] = line.astype(BF16)


def own_inject(m22, t22, w2, k21, i22, k21d):
    rows, cols, ch = m22.shape
    step = 4

    @pl.loop(0, rows // step)
    def _(i):
        at = pl.ds(i * step, step)
        value = inject(m22[at].reshape(step * cols, ch), t22[at].reshape(step * cols, ch), w2[...])
        i22[at] = value.reshape(step, cols, ch)

    half = k21.shape[1] // 9
    for t in range(9):
        tap = k21[:, t * half : (t + 1) * half].astype(F32)
        k21d[:, t * 128 : (t + 1) * 128] = jnp.concatenate([tap, tap], axis=1).astype(BF16)


def pack_cols(seeds, m32, m31, m22, i22, m21, a2, above, below, left, right, s256, s128, line, sa, flat):
    rows, cols, _ = seeds.shape
    for out, at_end in ((left, False), (right, True)):
        for source, base, row_base, width in (
            (seeds, COL_SEED, ROW_SEED, 4), (m32, COL_M32, ROW_M32, 3), (m31, COL_M31, ROW_M31, 2),
        ):
            c0 = cols - 16 if at_end else 0
            pick = 16 - width if at_end else 0
            for h in range(2):
                sl = slice(h * 128, (h + 1) * 128)
                own = source[:, c0 : c0 + 16, sl].astype(F32).reshape(rows * 16, 128)
                s256[width * 16 : (width + rows) * 16] = own
                for k in range(width):
                    at = row_base + (k * 2 + h) * cols + c0
                    s256[k * 16 : (k + 1) * 16] = above[at : at + 16].astype(F32)
                    low = (width + rows + k) * 16
                    s256[low : low + 16] = below[at : at + 16].astype(F32)
                for c in range(width):
                    to = base + (c * 2 + h) * 24
                    flat[to : to + 24] = s256[pl.ds(pick + c, 24, stride=16), :]
        tall, wide, _ = m22.shape
        c0 = wide - 16 if at_end else 0
        for source, base, row_base, width in (
            (m22, COL_M22, ROW_M22, 2), (i22, COL_I22, ROW_I22, 2), (m21, COL_M21, ROW_M21, 1),
        ):
            pick = 16 - width if at_end else 0
            own = source[:, c0 : c0 + 16].astype(F32).reshape(tall * 16, 128)
            s128[width * 16 : (width + tall) * 16] = own
            for k in range(width):
                at = row_base + k * wide + c0
                s128[k * 16 : (k + 1) * 16] = above[at : at + 16].astype(F32)
                low = (width + tall + k) * 16
                s128[low : low + 16] = below[at : at + 16].astype(F32)
            for c in range(width):
                to = base + c * 40
                flat[to : to + 40] = s128[pl.ds(pick + c, 40, stride=16), :]
        edge = cols - 1 if at_end else 0
        flat[COL_A2 + 1 : COL_A2 + 1 + rows] = a2[:, edge * 128 : (edge + 1) * 128].astype(F32)
        line[...] = above[ROW_A2 : ROW_A2 + cols].astype(F32)
        flat[COL_A2 : COL_A2 + 1] = line[edge : edge + 1]
        line[...] = below[ROW_A2 : ROW_A2 + cols].astype(F32)
        flat[COL_A2 + 1 + rows : COL_A2 + 2 + rows] = line[edge : edge + 1]
        out[...] = flat[...].astype(BF16)


def conv(x, kernel, row, count):
    width, amount = x.shape[1], x.shape[2]
    span = kernel.shape[1] // 3
    total = None
    for dy in range(3):
        block = x[pl.ds(row + 2 - dy, count)].reshape(count * width, amount)
        term = jnp.dot(block, kernel[:, dy * span : (dy + 1) * span], preferred_element_type=F32)
        total = term if total is None else total + term
    n = span // 3
    size = count * width
    before = pltpu.roll(total[:, :n], size - 1, 0)
    after = pltpu.roll(total[:, 2 * n :], 1, 0)
    return before + total[:, n : 2 * n] + after


def main(seeds, m32, m31, m22, i22, m21, a2, a1, above, below, fl, fr, k33, k32, k31, k22, k21d,
         result, e33, e32, e31, ea, e22, ei, e21, x33, x32, x31, u2, g22, g21, p1, o1):
    rows, cols, _ = seeds.shape
    tall, wide, _ = m22.shape

    for source, stage, row_base, col_base, width in (
        (seeds, e33, ROW_SEED, COL_SEED, 4), (m32, e32, ROW_M32, COL_M32, 3), (m31, e31, ROW_M31, COL_M31, 2),
    ):
        for h in range(2):
            sl = slice(h * 128, (h + 1) * 128)

            @pl.loop(0, rows)
            def _(r):
                to = pl.multiple_of((r + width) * W3 + LEAD, 8)
                stage[h, pl.ds(to, cols)] = source[r, :, sl].astype(F32)

            for k in range(width):
                at = row_base + (k * 2 + h) * cols
                to = k * W3 + LEAD
                stage[h, to : to + cols] = above[at : at + cols].astype(F32)
                to = (width + rows + k) * W3 + LEAD
                stage[h, to : to + cols] = below[at : at + cols].astype(F32)
            for c in range(width):
                at = col_base + (c * 2 + h) * 24
                stage.at[h][pl.ds(LEAD - width + c, 24, stride=W3), :] = fl[at : at + 24].astype(F32)
                stage.at[h][pl.ds(LEAD + cols + c, 24, stride=W3), :] = fr[at : at + 24].astype(F32)
    for source, stage, row_base, col_base, width in (
        (m22, e22, ROW_M22, COL_M22, 2), (i22, ei, ROW_I22, COL_I22, 2), (m21, e21, ROW_M21, COL_M21, 1),
    ):

        @pl.loop(0, tall)
        def _(r):
            to = pl.multiple_of((r + width) * W2 + LEAD, 8)
            stage[pl.ds(to, wide)] = source[r].astype(F32)

        for k in range(width):
            at = row_base + k * wide
            to = k * W2 + LEAD
            stage[to : to + wide] = above[at : at + wide].astype(F32)
            to = (width + tall + k) * W2 + LEAD
            stage[to : to + wide] = below[at : at + wide].astype(F32)
        for c in range(width):
            at = col_base + c * 40
            stage[pl.ds(LEAD - width + c, 40, stride=W2), :] = fl[at : at + 40].astype(F32)
            stage[pl.ds(LEAD + wide + c, 40, stride=W2), :] = fr[at : at + 40].astype(F32)
    for c in range(cols):
        ea[pl.ds(W3 + LEAD + c, rows, stride=W3), :] = a2[:, c * 128 : (c + 1) * 128].astype(F32)
    ea[LEAD : LEAD + cols] = above[ROW_A2 : ROW_A2 + cols].astype(F32)
    to = (rows + 1) * W3 + LEAD
    ea[to : to + cols] = below[ROW_A2 : ROW_A2 + cols].astype(F32)
    ea[pl.ds(LEAD - 1, 24, stride=W3), :] = fl[COL_A2 : COL_A2 + 24].astype(F32)
    ea[pl.ds(LEAD + cols, 24, stride=W3), :] = fr[COL_A2 : COL_A2 + 24].astype(F32)

    @pl.loop(0, rows + 8)
    def _(r):
        at = pl.ds(pl.multiple_of(r * W3, W3), W3)
        for h in range(2):
            x33[r, :, h * 128 : (h + 1) * 128] = e33[h, at].astype(BF16)

    for x, kernel, stage, nxt, count in ((x33, k33, e32, x32, 2), (x32, k32, e31, x31, 2)):

        @pl.loop(0, nxt.shape[0] // count)
        def _(i):
            row = i * count
            value = conv(x, kernel, row, count)
            at = pl.ds(pl.multiple_of(row * W3, W3), count * W3)
            for h in range(2):
                part = jnp.where(stage[h, at] > 0, value[:, h * 128 : (h + 1) * 128], 0.0)
                nxt[pl.ds(row, count), :, h * 128 : (h + 1) * 128] = part.astype(BF16).reshape(
                    count, W3, 128
                )

    @pl.loop(0, (rows + 2) // 3)
    def _(i):
        row = i * 3
        value = conv(x31, k31, row, 3)
        for k in range(3):
            part = value[k * W3 : (k + 1) * W3]
            where = ea[pl.ds(pl.multiple_of((row + k) * W3, W3), W3)]
            for a in range(2):
                for b in range(2):
                    to = (2 * (row + k) + a) * WU + b
                    u2[pl.ds(to, W3, stride=2), :] = jnp.where(where == 2.0 * a + b, part, 0.0)

    @pl.loop(0, tall + 4)
    def _(r):
        at = pl.ds(pl.multiple_of(r * W2, W2), W2)
        arriving = u2[pl.ds(pl.multiple_of(r * WU + LEAD, 8), W2)] + ei[at]
        g22[r] = jnp.where(e22[at] > 0, arriving, 0.0).astype(BF16)

    @pl.loop(0, (tall + 2) // 2)
    def _(i):
        row = i * 2
        value = conv(g22, k22, row, 2)
        value = jnp.where(e21[pl.ds(pl.multiple_of(row * W2, W2), 2 * W2)] > 0, value, 0.0)
        g21[pl.ds(row, 2)] = value.astype(BF16).reshape(2, W2, 128)

    @pl.loop(0, tall // 2)
    def _(i):
        row = i * 2
        value = conv(g21, k21d, row, 2)
        for k in range(2):
            to = pl.multiple_of((row + k) * WP, 8)
            p1[pl.ds(to, W2)] = value[k * W2 : (k + 1) * W2]

    lane = lax.broadcasted_iota(jnp.int32, (tall, 128), 1)
    high = lane >= 64
    shift = jnp.where(high, 1, 0)

    @pl.loop(0, wide // 2)
    def _(t):
        where = a1[:, pl.ds(pl.multiple_of(t * 128, 128), 128)]
        turned = pltpu.roll(where, 64, 1)
        for odd in range(2):
            spread = jnp.where(high, where, turned) if odd else jnp.where(high, turned, where)
            spread = spread - shift
            value = p1[pl.ds(LEAD + 2 * t + odd, tall, stride=WP), :]
            for a in range(2):
                o1.at[odd][pl.ds(a, tall, stride=2), :] = jnp.where(spread == 2 * a, value, 0.0)
            to = pl.ds(pl.multiple_of((2 * t + odd) * 128, 128), 128)
            result[:, to] = o1[odd].astype(BF16)


def whole(array):
    zeros = (0,) * array.ndim
    return pl.BlockSpec(array.shape, lambda i: zeros)


def call(body, args, outs, scratch=(), specs=None, cost=0):
    shapes = [jax.ShapeDtypeStruct(s, d) for s, d in outs]
    return pl.pallas_call(
        body,
        grid=(1,),
        in_specs=specs or [whole(a) for a in args],
        out_specs=[whole(s) for s in shapes],
        out_shape=shapes,
        scratch_shapes=[pltpu.VMEM(s, d) for s, d in scratch],
        cost_estimate=pl.CostEstimate(flops=cost, bytes_accessed=4000000, transcendentals=0),
        compiler_params=pltpu.CompilerParams(vmem_limit_bytes=50 << 20),
    )(*args)


def swap(first, last, axis):
    count = lax.axis_size(axis)
    from_before = lax.ppermute(last, axis, [(i, i + 1) for i in range(count - 1)])
    from_after = lax.ppermute(first, axis, [(i + 1, i) for i in range(count - 1)])
    return from_before, from_after


def shards(m21, m22, m31, m32, m33, t22, t33, a1, a2, w2, w3, k21, k22, k31, k32, k33):
    rows, cols, ch3 = m33.shape
    tall, wide, ch2 = m22.shape
    w2 = w2.reshape(1, ch2)
    w3 = w3.reshape(1, ch3)

    def band(height, index):
        return pl.BlockSpec((height, wide, ch2), lambda i: (index, 0, 0))

    args = (m33, t33, m32, m31, m22, m22, t22, t22, m21, m21, a2, w2, w3)
    specs = [whole(a) for a in args]
    specs[4], specs[5] = band(2, 0), band(2, tall // 2 - 1)
    specs[6], specs[7] = band(2, 0), band(2, tall // 2 - 1)
    specs[8], specs[9] = band(1, 0), band(1, tall - 1)
    seeds, up, down = call(
        pack_rows, args,
        [((rows, cols, ch3), BF16), ((ROW_TOTAL, 128), BF16), ((ROW_TOTAL, 128), BF16)],
        specs=specs, cost=10**9,
    )
    above, below = swap(up, down, "row")
    i22, k21d = call(
        own_inject, (m22, t22, w2, k21),
        [((tall, wide, ch2), F32), ((k21.shape[0], 9 * 128), BF16)], cost=10**9,
    )
    left, right = call(
        pack_cols, (seeds, m32, m31, m22, i22, m21, a2, above, below),
        [((COL_TOTAL, 128), BF16), ((COL_TOTAL, 128), BF16)],
        scratch=[((24 * 16, 128), F32), ((40 * 16, 128), F32), ((cols, 128), F32), ((8, 128), F32),
                 ((COL_TOTAL, 128), F32)],
        cost=10**9,
    )
    fl, fr = swap(left, right, "col")
    area3, area2 = (rows + 8) * W3, (tall + 8) * W2
    (result,) = call(
        main,
        (seeds, m32, m31, m22, i22, m21, a2, a1, above, below, fl, fr, k33, k32, k31, k22, k21d),
        [((2 * tall, 2 * wide * 64), BF16)],
        scratch=[
            ((2, area3, 128), F32), ((2, area3, 128), F32), ((2, area3, 128), F32), ((area3, 128), F32),
            ((area2, 128), F32), ((area2, 128), F32), ((area2, 128), F32),
            ((rows + 8, W3, ch3), BF16), ((rows + 6, W3, ch3), BF16), ((rows + 4, W3, ch3), BF16),
            (((tall + 4) * WU, 128), F32), ((tall + 4, W2, ch2), BF16), ((tall + 2, W2, ch2), BF16),
            ((tall * WP, 128), F32), ((2, 2 * tall, 128), F32),
        ],
        cost=3 * 10**9,
    )
    return result


def solution(mesh):
    in_specs = (P("row", "col", None),) * 7 + (P("row", "col"),) * 2 + (P(),) * 7
    return jax.shard_map(
        shards, mesh=mesh, in_specs=in_specs, out_specs=P("row", "col"), check_vma=False
    )
```

```python
import jax
import jax.numpy as jnp
from jax import lax
from jax.experimental import pallas as pl
from jax.experimental.pallas import tpu as pltpu
from jax.sharding import PartitionSpec as P

EPSILON = 1e-06
F32 = jnp.float32
BF16 = jnp.bfloat16

ROW_SEED, ROW_M32, ROW_M31, ROW_M22, ROW_I22, ROW_M21, ROW_A2, ROW_TOTAL = (
    0, 256, 448, 576, 704, 832, 896, 928)
COL_SEED, COL_M32, COL_M31, COL_M22, COL_I22, COL_M21, COL_A2, COL_TOTAL = (
    0, 192, 336, 432, 512, 592, 632, 656)
W3 = 48
W2 = 80
WU = 96
WP = 88
LEAD = 8
N33, N32, N31, N22, N21 = 11, 10, 9, 17, 16
LIM = (8, 8, 8, 30)


def inject(preact, target, weight):
    count = preact.shape[-1]
    feature = jnp.maximum(preact.astype(F32), 0.0)
    wanted = jnp.maximum(target.astype(F32), 0.0)
    scale = lax.rsqrt(jnp.sum(feature * feature, axis=-1, keepdims=True) * (1.0 / count) + EPSILON)
    other = lax.rsqrt(jnp.sum(wanted * wanted, axis=-1, keepdims=True) * (1.0 / count) + EPSILON)
    scaled = feature * scale
    excess = (2.0 * weight) * (scaled - wanted * other)
    mean = jnp.sum(excess * scaled, axis=-1, keepdims=True) * (1.0 / count)
    return (excess - scaled * mean) * scale


def pack_rows(hm33, ht33, hm32, hm31, hm22, ht22, hm21, ha2, hw2, hw3, seeds, up, down,
              m33, t33, m32, m31, m22e, t22e, m21e, a2, w2, w3, sems):
    rows, cols, ch = m33.shape
    tall = hm22.shape[0]
    moves = []
    for source, target in (
        (hm33.at[0:8], m33.at[0:8]), (ht33.at[0:8], t33.at[0:8]),
        (hm33.at[8:rows], m33.at[8:rows]), (ht33.at[8:rows], t33.at[8:rows]),
        (hm22.at[0:2], m22e.at[0]), (hm22.at[tall - 2 : tall], m22e.at[1]),
        (ht22.at[0:2], t22e.at[0]), (ht22.at[tall - 2 : tall], t22e.at[1]),
        (hm32.at[0:3], m32.at[0:3]), (hm32.at[rows - 3 : rows], m32.at[3:6]),
        (hm31.at[0:2], m31.at[0:2]), (hm31.at[rows - 2 : rows], m31.at[2:4]),
        (hm21.at[0], m21e.at[0]), (hm21.at[tall - 1], m21e.at[1]),
        (ha2, a2), (hw2, w2), (hw3, w3),
    ):
        moves.append(pltpu.make_async_copy(source, target, sems.at[len(moves)]))
        moves[-1].start()
    for move in moves:
        move.wait()
    step = 4
    for r in range(0, rows, step):
        p = m33[r : r + step].reshape(step * cols, ch)
        value = inject(p, t33[r : r + step].reshape(step * cols, ch), w3[...])
        value = jnp.where(p.astype(F32) > 0, value, 0.0).astype(BF16)
        seeds[r : r + step] = value.reshape(step, cols, ch)
    for out, side, edge in ((up, 0, 0), (down, 1, rows - 1)):
        m22, t22 = m22e.at[side], t22e.at[side]
        for source, base, width, begin in (
            (seeds, ROW_SEED, 4, side * (rows - 4)), (m32, ROW_M32, 3, side * 3), (m31, ROW_M31, 2, side * 2),
        ):
            for k in range(width):
                for h in range(2):
                    at = base + (k * 2 + h) * cols
                    out[at : at + cols] = source[begin + k, :, h * 128 : (h + 1) * 128]
        wide = m22.shape[1]
        p = m22[...].reshape(2 * wide, 128)
        out[ROW_M22 : ROW_M22 + 2 * wide] = p
        out[ROW_I22 : ROW_I22 + 2 * wide] = inject(
            p, t22[...].reshape(2 * wide, 128), w2[...]
        ).astype(BF16)
        out[ROW_M21 : ROW_M21 + wide] = m21e[side]
        line = a2[edge : edge + 1, :].astype(F32)
        line = jnp.concatenate([line[:, c * 128 : (c + 1) * 128] for c in range(cols)], axis=0)
        out[ROW_A2 : ROW_A2 + cols] = line.astype(BF16)


def own_inject(m22, t22, w2, k21, i22, k21d):
    rows, cols, ch = m22.shape
    step = 4

    @pl.loop(0, rows // step)
    def _(i):
        at = pl.ds(i * step, step)
        value = inject(m22[at].reshape(step * cols, ch), t22[at].reshape(step * cols, ch), w2[...])
        i22[at] = value.reshape(step, cols, ch)

    half = k21.shape[0] // 9
    for t in range(9):
        tap = k21[t * half : (t + 1) * half].astype(F32)
        k21d[:, t * 128 : (t + 1) * 128] = jnp.concatenate([tap, tap], axis=0).T.astype(BF16)


def pack_cols(seeds, m32, m31, m22, i22, m21, a2, above, below, left, right, s256, s128, line, sa, flat):
    rows, cols, _ = seeds.shape
    for out, at_end in ((left, False), (right, True)):
        for source, base, row_base, width in (
            (seeds, COL_SEED, ROW_SEED, 4), (m32, COL_M32, ROW_M32, 3), (m31, COL_M31, ROW_M31, 2),
        ):
            c0 = cols - 16 if at_end else 0
            pick = 16 - width if at_end else 0
            for h in range(2):
                sl = slice(h * 128, (h + 1) * 128)
                own = source[:, c0 : c0 + 16, sl].astype(F32).reshape(rows * 16, 128)
                s256[width * 16 : (width + rows) * 16] = own
                for k in range(width):
                    at = row_base + (k * 2 + h) * cols + c0
                    s256[k * 16 : (k + 1) * 16] = above[at : at + 16].astype(F32)
                    low = (width + rows + k) * 16
                    s256[low : low + 16] = below[at : at + 16].astype(F32)
                for c in range(width):
                    to = base + (c * 2 + h) * 24
                    flat[to : to + 24] = s256[pl.ds(pick + c, 24, stride=16), :]
        tall, wide, _ = m22.shape
        c0 = wide - 16 if at_end else 0
        for source, base, row_base, width in (
            (m22, COL_M22, ROW_M22, 2), (i22, COL_I22, ROW_I22, 2), (m21, COL_M21, ROW_M21, 1),
        ):
            pick = 16 - width if at_end else 0
            own = source[:, c0 : c0 + 16].astype(F32).reshape(tall * 16, 128)
            s128[width * 16 : (width + tall) * 16] = own
            for k in range(width):
                at = row_base + k * wide + c0
                s128[k * 16 : (k + 1) * 16] = above[at : at + 16].astype(F32)
                low = (width + tall + k) * 16
                s128[low : low + 16] = below[at : at + 16].astype(F32)
            for c in range(width):
                to = base + c * 40
                flat[to : to + 40] = s128[pl.ds(pick + c, 40, stride=16), :]
        edge = cols - 1 if at_end else 0
        flat[COL_A2 + 1 : COL_A2 + 1 + rows] = a2[:, edge * 128 : (edge + 1) * 128].astype(F32)
        line[...] = above[ROW_A2 : ROW_A2 + cols].astype(F32)
        flat[COL_A2 : COL_A2 + 1] = line[edge : edge + 1]
        line[...] = below[ROW_A2 : ROW_A2 + cols].astype(F32)
        flat[COL_A2 + 1 + rows : COL_A2 + 2 + rows] = line[edge : edge + 1]
        out[...] = flat[...].astype(BF16)


def conv(x, kernel, row, count):
    width, amount = x.shape[1], x.shape[2]
    span = kernel.shape[1] // 3
    total = None
    for dy in range(3):
        block = x[pl.ds(row + 2 - dy, count)].reshape(count * width, amount)
        term = jnp.dot(block, kernel[:, dy * span : (dy + 1) * span], preferred_element_type=F32)
        total = term if total is None else total + term
    n = span // 3
    size = count * width
    before = pltpu.roll(total[:, :n], size - 1, 0)
    after = pltpu.roll(total[:, 2 * n :], 1, 0)
    return before + total[:, n : 2 * n] + after


def main(seeds, m32, m31, m22, i22, m21, a2, a1, above, below, fl, fr, k33, k32, k31, k22, k21d,
         result, e33, e32, e31, ea, e22, ei, e21, x33, x32, x31, u2, g22, g21, p1, o1):
    rows, cols, _ = seeds.shape
    tall, wide, _ = m22.shape

    for source, stage, row_base, col_base, width in (
        (seeds, e33, ROW_SEED, COL_SEED, 4), (m32, e32, ROW_M32, COL_M32, 3), (m31, e31, ROW_M31, COL_M31, 2),
    ):
        for h in range(2):
            sl = slice(h * 128, (h + 1) * 128)

            @pl.loop(0, rows)
            def _(r):
                to = pl.multiple_of((r + width) * W3 + LEAD, 8)
                stage[h, pl.ds(to, cols)] = source[r, :, sl].astype(F32)

            for k in range(width):
                at = row_base + (k * 2 + h) * cols
                to = k * W3 + LEAD
                stage[h, to : to + cols] = above[at : at + cols].astype(F32)
                to = (width + rows + k) * W3 + LEAD
                stage[h, to : to + cols] = below[at : at + cols].astype(F32)
            for c in range(width):
                at = col_base + (c * 2 + h) * 24
                stage.at[h][pl.ds(LEAD - width + c, 24, stride=W3), :] = fl[at : at + 24].astype(F32)
                stage.at[h][pl.ds(LEAD + cols + c, 24, stride=W3), :] = fr[at : at + 24].astype(F32)
    for source, stage, row_base, col_base, width in (
        (m22, e22, ROW_M22, COL_M22, 2), (i22, ei, ROW_I22, COL_I22, 2), (m21, e21, ROW_M21, COL_M21, 1),
    ):

        @pl.loop(0, tall)
        def _(r):
            to = pl.multiple_of((r + width) * W2 + LEAD, 8)
            stage[pl.ds(to, wide)] = source[r].astype(F32)

        for k in range(width):
            at = row_base + k * wide
            to = k * W2 + LEAD
            stage[to : to + wide] = above[at : at + wide].astype(F32)
            to = (width + tall + k) * W2 + LEAD
            stage[to : to + wide] = below[at : at + wide].astype(F32)
        for c in range(width):
            at = col_base + c * 40
            stage[pl.ds(LEAD - width + c, 40, stride=W2), :] = fl[at : at + 40].astype(F32)
            stage[pl.ds(LEAD + wide + c, 40, stride=W2), :] = fr[at : at + 40].astype(F32)
    for c in range(cols):
        ea[pl.ds(W3 + LEAD + c, rows, stride=W3), :] = a2[:, c * 128 : (c + 1) * 128].astype(F32)
    ea[LEAD : LEAD + cols] = above[ROW_A2 : ROW_A2 + cols].astype(F32)
    to = (rows + 1) * W3 + LEAD
    ea[to : to + cols] = below[ROW_A2 : ROW_A2 + cols].astype(F32)
    ea[pl.ds(LEAD - 1, 24, stride=W3), :] = fl[COL_A2 : COL_A2 + 24].astype(F32)
    ea[pl.ds(LEAD + cols, 24, stride=W3), :] = fr[COL_A2 : COL_A2 + 24].astype(F32)

    @pl.loop(0, rows + 8)
    def _(r):
        at = pl.ds(pl.multiple_of(r * W3, W3), W3)
        for h in range(2):
            x33[r, :, h * 128 : (h + 1) * 128] = e33[h, at].astype(BF16)

    for x, kernel, stage, nxt, count in ((x33, k33, e32, x32, N33), (x32, k32, e31, x31, N32)):

        @pl.loop(0, nxt.shape[0] // count)
        def _(i):
            row = i * count
            value = conv(x, kernel, row, count)
            at = pl.ds(pl.multiple_of(row * W3, W3), count * W3)
            for h in range(2):
                part = jnp.where(stage[h, at] > 0, value[:, h * 128 : (h + 1) * 128], 0.0)
                nxt[pl.ds(row, count), :, h * 128 : (h + 1) * 128] = part.astype(BF16).reshape(
                    count, W3, 128
                )

    @pl.loop(0, (rows + 2) // N31)
    def _(i):
        row = i * N31
        value = conv(x31, k31, row, N31)
        for k in range(N31):
            part = value[k * W3 : (k + 1) * W3]
            where = ea[pl.ds(pl.multiple_of((row + k) * W3, W3), W3)]
            for a in range(2):
                for b in range(2):
                    to = (2 * (row + k) + a) * WU + b
                    u2[pl.ds(to, W3, stride=2), :] = jnp.where(where == 2.0 * a + b, part, 0.0)

    @pl.loop(0, tall + 4)
    def _(r):
        at = pl.ds(pl.multiple_of(r * W2, W2), W2)
        arriving = u2[pl.ds(pl.multiple_of(r * WU + LEAD, 8), W2)] + ei[at]
        g22[r] = jnp.where(e22[at] > 0, arriving, 0.0).astype(BF16)

    @pl.loop(0, (tall + 2) // N22)
    def _(i):
        row = i * N22
        value = conv(g22, k22, row, N22)
        value = jnp.where(e21[pl.ds(pl.multiple_of(row * W2, W2), N22 * W2)] > 0, value, 0.0)
        g21[pl.ds(row, N22)] = value.astype(BF16).reshape(N22, W2, 128)

    @pl.loop(0, tall // N21)
    def _(i):
        row = i * N21
        value = conv(g21, k21d, row, N21)
        for k in range(N21):
            to = pl.multiple_of((row + k) * WP, 8)
            p1[pl.ds(to, W2)] = value[k * W2 : (k + 1) * W2]

    lane = lax.broadcasted_iota(jnp.int32, (tall, 128), 1)
    high = lane >= 64
    shift = jnp.where(high, 1, 0)

    @pl.loop(0, wide // 2)
    def _(t):
        where = a1[:, pl.ds(pl.multiple_of(t * 128, 128), 128)]
        turned = pltpu.roll(where, 64, 1)
        for odd in range(2):
            spread = jnp.where(high, where, turned) if odd else jnp.where(high, turned, where)
            spread = spread - shift
            value = p1[pl.ds(LEAD + 2 * t + odd, tall, stride=WP), :]
            for a in range(2):
                o1.at[odd][pl.ds(a, tall, stride=2), :] = jnp.where(spread == 2 * a, value, 0.0)
            to = pl.ds(pl.multiple_of((2 * t + odd) * 128, 128), 128)
            result[:, to] = o1[odd].astype(BF16)


def whole(array):
    zeros = (0,) * array.ndim
    return pl.BlockSpec(array.shape, lambda i: zeros)


def call(body, args, outs, scratch=(), specs=None, cost=0, limit=8):
    shapes = [jax.ShapeDtypeStruct(s, d) for s, d in outs]
    return pl.pallas_call(
        body,
        grid=(1,),
        in_specs=specs or [whole(a) for a in args],
        out_specs=[whole(s) for s in shapes],
        out_shape=shapes,
        scratch_shapes=[pltpu.VMEM(*s) if isinstance(s, tuple) else s for s in scratch],
        cost_estimate=pl.CostEstimate(flops=cost, bytes_accessed=4000000, transcendentals=0),
        compiler_params=pltpu.CompilerParams(vmem_limit_bytes=limit << 20),
    )(*args)


def swap(first, last, axis):
    count = lax.axis_size(axis)
    from_before = lax.ppermute(last, axis, [(i, i + 1) for i in range(count - 1)])
    from_after = lax.ppermute(first, axis, [(i + 1, i) for i in range(count - 1)])
    return from_before, from_after


def shards(m21, m22, m31, m32, m33, t22, t33, a1, a2, w2, w3, k21, k22, k31, k32, k33):
    rows, cols, ch3 = m33.shape
    tall, wide, ch2 = m22.shape
    w2 = w2.reshape(1, ch2)
    w3 = w3.reshape(1, ch3)

    stored = pl.BlockSpec(memory_space=pltpu.MemorySpace.HBM)
    args = tuple(pltpu.with_memory_space_constraint(x, pltpu.MemorySpace.HBM) for x in (m33, t33, m32, m31, m22, t22, m21, a2, w2, w3))
    seeds, up, down = call(
        pack_rows, args,
        [((rows, cols, ch3), BF16), ((ROW_TOTAL, 128), BF16), ((ROW_TOTAL, 128), BF16)],
        scratch=[
            ((rows, cols, ch3), BF16), ((rows, cols, ch3), BF16), ((6, cols, ch3), BF16),
            ((4, cols, ch3), BF16), ((2, 2, wide, ch2), BF16), ((2, 2, wide, ch2), BF16),
            ((2, wide, ch2), BF16), (a2.shape, a2.dtype), (w2.shape, F32), (w3.shape, F32),
            pltpu.SemaphoreType.DMA((17,)),
        ],
        specs=[stored] * 10, cost=10**9, limit=LIM[0],
    )
    above, below = swap(up, down, "row")
    i22, k21d = call(
        own_inject, (m22, t22, w2, k21.T),
        [((tall, wide, ch2), F32), ((k21.shape[0], 9 * 128), BF16)], cost=10**9, limit=LIM[1],
    )
    left, right = call(
        pack_cols, (seeds, m32, m31, m22, i22, m21, a2, above, below),
        [((COL_TOTAL, 128), BF16), ((COL_TOTAL, 128), BF16)],
        scratch=[((24 * 16, 128), F32), ((40 * 16, 128), F32), ((cols, 128), F32), ((8, 128), F32),
                 ((COL_TOTAL, 128), F32)],
        cost=10**9, limit=LIM[2],
    )
    fl, fr = swap(left, right, "col")
    area3, area2 = (rows + 8) * W3, (tall + 8) * W2
    (result,) = call(
        main,
        (seeds, m32, m31, m22, i22, m21, a2, a1, above, below, fl, fr, k33, k32, k31, k22, k21d),
        [((2 * tall, 2 * wide * 64), BF16)],
        scratch=[
            ((2, area3, 128), F32), ((2, area3, 128), F32), ((2, area3, 128), F32), ((area3, 128), F32),
            ((area2, 128), F32), ((area2, 128), F32), ((area2, 128), F32),
            ((rows + 8, W3, ch3), BF16), ((rows + 6, W3, ch3), BF16), ((rows + 4, W3, ch3), BF16),
            (((tall + 4) * WU, 128), F32), ((tall + 4, W2, ch2), BF16), ((tall + 2, W2, ch2), BF16),
            ((tall * WP, 128), F32), ((2, 2 * tall, 128), F32),
        ],
        cost=3 * 10**9, limit=LIM[3],
    )
    return result


def solution(mesh):
    in_specs = (P("row", "col", None),) * 7 + (P("row", "col"),) * 2 + (P(),) * 7
    return jax.shard_map(
        shards, mesh=mesh, in_specs=in_specs, out_specs=P("row", "col"), check_vma=False
    )
```

```python
import jax
import jax.numpy as jnp
from jax import lax
from jax.experimental import pallas as pl
from jax.experimental.pallas import tpu as pltpu
from jax.sharding import PartitionSpec as P

EPSILON = 1e-06
F32 = jnp.float32
BF16 = jnp.bfloat16

COL_SEED, COL_M32, COL_M31, COL_M22, COL_I22, COL_M21, COL_A2, COL_TOTAL = (
    0, 128, 224, 288, 352, 416, 448, 464)
ROW_SEED, ROW_M32, ROW_M31, ROW_A2, ROW_M22, ROW_I22, ROW_M21, ROW_TOTAL = (
    0, 320, 560, 720, 760, 904, 1048, 1120)
T3, T2 = 40, 72
W3, W2, WU, WP = 48, 80, 96, 88
LEAD = 8
LIM = (8, 8, 8, 26, 26)


def inject(preact, target, weight):
    count = preact.shape[-1]
    feature = jnp.maximum(preact.astype(F32), 0.0)
    wanted = jnp.maximum(target.astype(F32), 0.0)
    scale = lax.rsqrt(jnp.sum(feature * feature, axis=-1, keepdims=True) * (1.0 / count) + EPSILON)
    other = lax.rsqrt(jnp.sum(wanted * wanted, axis=-1, keepdims=True) * (1.0 / count) + EPSILON)
    scaled = feature * scale
    excess = (2.0 * weight) * (scaled - wanted * other)
    mean = jnp.sum(excess * scaled, axis=-1, keepdims=True) * (1.0 / count)
    return (excess - scaled * mean) * scale


def pack_cols(hm33, ht33, hm32, hm31, hm22, ht22, hm21, ha2, hw2, hw3, seeds, left, right,
              m33, t33, m32, m31, m22, t22, m21, a2, w2, w3, st3, st2, flat, sems):
    rows, cols, ch = m33.shape
    tall, wide, _ = hm22.shape
    moves = []
    for source, target in (
        (hm33.at[0:8], m33.at[0:8]), (ht33.at[0:8], t33.at[0:8]),
        (hm33.at[8:rows], m33.at[8:rows]), (ht33.at[8:rows], t33.at[8:rows]),
        (hm22.at[:, 0:8], m22.at[0]), (hm22.at[:, wide - 8 : wide], m22.at[1]),
        (ht22.at[:, 0:8], t22.at[0]), (ht22.at[:, wide - 8 : wide], t22.at[1]),
        (hm32.at[:, 0:8], m32.at[0]), (hm32.at[:, cols - 8 : cols], m32.at[1]),
        (hm31.at[:, 0:8], m31.at[0]), (hm31.at[:, cols - 8 : cols], m31.at[1]),
        (hm21.at[:, 0:8], m21.at[0]), (hm21.at[:, wide - 8 : wide], m21.at[1]),
        (ha2.at[:, 0:128], a2.at[0]), (ha2.at[:, (cols - 1) * 128 : cols * 128], a2.at[1]),
        (hw2, w2), (hw3, w3),
    ):
        moves.append(pltpu.make_async_copy(source, target, sems.at[len(moves)]))
        moves[-1].start()
    for move in moves:
        move.wait()
    step = 4
    for r in range(0, rows, step):
        p = m33[r : r + step].reshape(step * cols, ch)
        value = inject(p, t33[r : r + step].reshape(step * cols, ch), w3[...])
        value = jnp.where(p.astype(F32) > 0, value, 0.0).astype(BF16)
        seeds[r : r + step] = value.reshape(step, cols, ch)
    for side, out in enumerate((left, right)):
        edge = slice(cols - 8, cols) if side else slice(0, 8)
        for g, (base, width) in enumerate(((COL_SEED, 4), (COL_M32, 3), (COL_M31, 2))):
            pick = 8 - width if side else 0
            for h in range(2):
                lanes = slice(h * 128, (h + 1) * 128)
                own = (seeds[:, edge, lanes], m32[side, :, :, lanes], m31[side, :, :, lanes])[g]
                stage = st3.at[(g * 2 + side) * 2 + h]
                stage[...] = own.astype(F32).reshape(rows * 8, 128)
                for c in range(width):
                    to = base + (c * 2 + h) * rows
                    flat[side, to : to + rows] = stage[pl.ds(pick + c, rows, stride=8), :]
        p = m22[side].reshape(tall * 8, 128)
        groups = (
            (COL_M22, 2, p.astype(F32)),
            (COL_I22, 2, inject(p, t22[side].reshape(tall * 8, 128), w2[...])),
            (COL_M21, 1, m21[side].astype(F32).reshape(tall * 8, 128)),
        )
        for g, (base, width, own) in enumerate(groups):
            pick = 8 - width if side else 0
            stage = st2.at[g * 2 + side]
            stage[...] = own
            for c in range(width):
                to = base + c * tall
                flat[side, to : to + tall] = stage[pl.ds(pick + c, tall, stride=8), :]
        flat[side, COL_A2 : COL_A2 + rows] = a2[side].astype(F32)
        out[...] = flat[side].astype(BF16)

def own_inject(m22, t22, w2, k21, i22, k21d):
    rows, cols, ch = m22.shape
    step = 4

    @pl.loop(0, rows // step)
    def _(i):
        at = pl.ds(i * step, step)
        value = inject(m22[at].reshape(step * cols, ch), t22[at].reshape(step * cols, ch), w2[...])
        i22[at] = value.reshape(step, cols, ch)

    half = k21.shape[0] // 9
    for t in range(9):
        tap = k21[t * half : (t + 1) * half].astype(F32)
        k21d[:, t * 128 : (t + 1) * 128] = jnp.concatenate([tap, tap], axis=0).T.astype(BF16)


def pack_rows(seeds, m32, m31, m22, i22, m21, a2, fl, fr, up, down, side_l, side_r, flat):
    rows, cols, _ = seeds.shape
    tall, wide, _ = m22.shape
    side_l[...] = fl[...].astype(F32)
    side_r[...] = fr[...].astype(F32)
    for side, out in enumerate((up, down)):
        for source, base, col_base, width in (
            (seeds, ROW_SEED, COL_SEED, 4), (m32, ROW_M32, COL_M32, 3), (m31, ROW_M31, COL_M31, 2),
        ):
            r0 = rows - width if side else 0
            for h in range(2):
                for k in range(width):
                    to = base + (k * 2 + h) * T3 + 4
                    flat[side, to : to + cols] = source[r0 + k, :, h * 128 : (h + 1) * 128].astype(F32)
                for c in range(width):
                    at = col_base + (c * 2 + h) * rows + r0
                    to = base + h * T3
                    flat.at[side][pl.ds(to + 4 - width + c, width, stride=2 * T3), :] = side_l[at : at + width]
                    flat.at[side][pl.ds(to + 4 + cols + c, width, stride=2 * T3), :] = side_r[at : at + width]
        for source, base, col_base, width in (
            (m22, ROW_M22, COL_M22, 2), (i22, ROW_I22, COL_I22, 2), (m21, ROW_M21, COL_M21, 1),
        ):
            r0 = tall - width if side else 0
            for k in range(width):
                to = base + k * T2 + 4
                flat[side, to : to + wide] = source[r0 + k].astype(F32)
                for c in range(width):
                    at = col_base + c * tall + r0 + k
                    flat[side, to - width + c : to - width + c + 1] = side_l[at : at + 1]
                    flat[side, to + wide + c : to + wide + c + 1] = side_r[at : at + 1]
        r0 = rows - 1 if side else 0
        line = a2[r0 : r0 + 1, :].astype(F32)
        to = ROW_A2 + 4
        for c in range(cols):
            flat[side, to + c : to + c + 1] = line[:, c * 128 : (c + 1) * 128]
        at = COL_A2 + r0
        flat[side, to - 1 : to] = side_l[at : at + 1]
        flat[side, to + cols : to + cols + 1] = side_r[at : at + 1]
        out[...] = flat[side].astype(BF16)


def conv(pick, kernel):
    span = kernel.shape[1] // 3
    total = None
    for dy in range(3):
        term = jnp.dot(pick(dy), kernel[:, dy * span : (dy + 1) * span], preferred_element_type=F32)
        total = term if total is None else total + term
    n = span // 3
    before = pltpu.roll(total[:, :n], total.shape[0] - 1, 0)
    after = pltpu.roll(total[:, 2 * n :], 1, 0)
    return before + total[:, n : 2 * n] + after


def block(x, row, count):
    def pick(dy):
        return x[pl.ds(row + 2 - dy, count)].reshape(count * x.shape[1], x.shape[2])

    return pick


def spread(part, where, u2, row):
    for a in range(2):
        for b in range(2):
            to = (2 * row + a) * WU + b
            u2[pl.ds(to, W3, stride=2), :] = jnp.where(where == 2.0 * a + b, part, 0.0)


def emit(a1, pieces, o1):
    tiles = a1.shape[1] // 128
    group = 4

    @pl.loop(0, tiles // group)
    def _(i):
        for first, count, p1, out in pieces:
            high = lax.broadcasted_iota(jnp.int32, (count, 128), 1) >= 64
            shift = jnp.where(high, 1, 0)
            for j in range(group):
                t = i * group + j
                where = a1[first : first + count, pl.ds(pl.multiple_of(t * 128, 128), 128)]
                turned = pltpu.roll(where, 64, 1)
                for odd in range(2):
                    own = (jnp.where(high, where, turned) if odd else jnp.where(high, turned, where)) - shift
                    value = p1[pl.ds(LEAD + 2 * t + odd, count, stride=WP), :]
                    slot = o1.at[2 * j + odd]
                    for a in range(2):
                        slot[pl.ds(a, count, stride=2), :] = jnp.where(own == 2 * a, value, 0.0)
                    to = pl.ds(pl.multiple_of((2 * t + odd) * 128, 128), 128)
                    out[:, to] = slot[0 : 2 * count].astype(BF16)


def inner(seeds, m32, m31, m22, i22, m21, a2, a1, fl, fr, k33, k32, k31, k22, k21d,
          result, t33, t32, t31, ta, t22, ti, t21, y32, y31, y22, y21,
          e33, e32, e31, ea, e22, ei, e21, x33, x32, x31, u2, g22, g21, p1, o1, obuf, sem):
    rows, cols, _ = seeds.shape
    tall, wide, _ = m22.shape
    for source, stage, col_base, width in (
        (seeds, e33, COL_SEED, 4), (m32, e32, COL_M32, 3), (m31, e31, COL_M31, 2),
    ):

        @pl.loop(0, rows // 4)
        def _(i):
            for j in range(4):
                r = i * 4 + j
                to = pl.multiple_of(r * W3 + LEAD, 8)
                for h in range(2):
                    stage[h, pl.ds(to, cols)] = source[r, :, h * 128 : (h + 1) * 128].astype(F32)

        for h in range(2):
            for c in range(width):
                at = col_base + (c * 2 + h) * rows
                stage.at[h][pl.ds(LEAD - width + c, rows, stride=W3), :] = fl[at : at + rows].astype(F32)
                stage.at[h][pl.ds(LEAD + cols + c, rows, stride=W3), :] = fr[at : at + rows].astype(F32)
    for source, stage, col_base, width in (
        (m22, e22, COL_M22, 2), (i22, ei, COL_I22, 2), (m21, e21, COL_M21, 1),
    ):

        @pl.loop(0, tall // 4)
        def _(i):
            for j in range(4):
                r = i * 4 + j
                stage[pl.ds(pl.multiple_of(r * W2 + LEAD, 8), wide)] = source[r].astype(F32)

        for c in range(width):
            at = col_base + c * tall
            stage[pl.ds(LEAD - width + c, tall, stride=W2), :] = fl[at : at + tall].astype(F32)
            stage[pl.ds(LEAD + wide + c, tall, stride=W2), :] = fr[at : at + tall].astype(F32)
    for c in range(cols):
        ea[pl.ds(LEAD + c, rows, stride=W3), :] = a2[:, c * 128 : (c + 1) * 128].astype(F32)
    ea[pl.ds(LEAD - 1, rows, stride=W3), :] = fl[COL_A2 : COL_A2 + rows].astype(F32)
    ea[pl.ds(LEAD + cols, rows, stride=W3), :] = fr[COL_A2 : COL_A2 + rows].astype(F32)

    @pl.loop(0, rows // 2)
    def _(i):
        for j in range(2):
            at = pl.ds(pl.multiple_of((i * 2 + j) * W3, W3), W3)
            for h in range(2):
                x33[i * 2 + j, :, h * 128 : (h + 1) * 128] = e33[h, at].astype(BF16)

    for x, kernel, stage, nxt, skip in ((x33, k33, e32, x32, 1), (x32, k32, e31, x31, 2)):
        count = nxt.shape[0] // 2

        @pl.loop(0, 2)
        def _(i):
            row = i * count
            value = conv(block(x, row, count), kernel)
            at = pl.ds(pl.multiple_of((row + skip) * W3, W3), count * W3)
            for h in range(2):
                part = jnp.where(stage[h, at] > 0, value[:, h * 128 : (h + 1) * 128], 0.0)
                nxt[pl.ds(row, count), :, h * 128 : (h + 1) * 128] = part.astype(BF16).reshape(
                    count, W3, 128
                )

    count = (rows - 6) // 2

    @pl.loop(0, 2)
    def _(i):
        row = i * count
        value = conv(block(x31, row, count), k31)
        for k in range(count):
            where = ea[pl.ds(pl.multiple_of((row + k + 3) * W3, W3), W3)]
            spread(value[k * W3 : (k + 1) * W3], where, u2, row + k)

    @pl.loop(0, g22.shape[0] // 2)
    def _(i):
        for j in range(2):
            r = i * 2 + j
            at = pl.ds(pl.multiple_of((r + 6) * W2, W2), W2)
            arriving = u2[pl.ds(pl.multiple_of(r * WU + LEAD, 8), W2)] + ei[at]
            g22[r] = jnp.where(e22[at] > 0, arriving, 0.0).astype(BF16)

    count = g21.shape[0] // 2

    @pl.loop(0, 2)
    def _(i):
        row = i * count
        value = conv(block(g22, row, count), k22)
        at = pl.ds(pl.multiple_of((row + 7) * W2, W2), count * W2)
        value = jnp.where(e21[at] > 0, value, 0.0)
        g21[pl.ds(row, count)] = value.astype(BF16).reshape(count, W2, 128)

    half = (tall - 16) // 2

    @pl.loop(0, 2)
    def _(i):
        row = i * half
        value = conv(block(g21, row, half), k21d)
        for k in range(half):
            p1[pl.ds(pl.multiple_of((row + k) * WP, 8), W2)] = value[k * W2 : (k + 1) * W2]

    emit(a1, ((8, tall - 16, p1, obuf),), o1)
    move = pltpu.make_async_copy(obuf, result.at[16 : 2 * tall - 16], sem)
    move.start()
    for side in range(2):
        for target, stage, count, width in (
            (t33, e33, 2, W3), (t32, e32, 1, W3), (t31, e31, 2, W3),
        ):
            r0 = (rows - count) * side
            target[side] = stage[:, r0 * width : (r0 + count) * width]
        for target, stage, count, width, total in (
            (ta, ea, 3, W3, rows), (t22, e22, 6, W2, tall), (ti, ei, 6, W2, tall), (t21, e21, 7, W2, tall),
        ):
            r0 = (total - count) * side
            target[side] = stage[r0 * width : (r0 + count) * width]
        for target, source in ((y32, x32), (y31, x31), (y22, g22), (y21, g21)):
            r0 = (source.shape[0] - 2) * side
            target[side] = source[r0 : r0 + 2]
    move.wait()


def outer(t33, t32, t31, ta, t22, ti, t21, y32, y31, y22, y21, above, below, a1,
          k33, k32, k31, k22, k21d, partial, result,
          halo, e33, e32, e31, ea, e22, ei, e21, x33, x32, x31, u2, g22, g21, p1, o1, obuf, sem):
    del partial
    tall = result.shape[0] // 2
    halo[0] = above[...].astype(F32)
    halo[1] = below[...].astype(F32)
    for side in range(2):
        for own, stage, base, width in (
            (t33, e33, ROW_SEED, 4), (t32, e32, ROW_M32, 3), (t31, e31, ROW_M31, 2),
        ):
            keep = own.shape[2]
            for h in range(2):
                to = 0 if side else width * W3
                stage[side, h, to : to + keep] = own[side, h]
                for k in range(width):
                    at = base + (k * 2 + h) * T3
                    to = k * W3 + 4 + (keep if side else 0)
                    stage[side, h, to : to + T3] = halo[side, at : at + T3]
        for own, stage, base, width, narrow, full in (
            (ta, ea, ROW_A2, 1, T3, W3), (t22, e22, ROW_M22, 2, T2, W2),
            (ti, ei, ROW_I22, 2, T2, W2), (t21, e21, ROW_M21, 1, T2, W2),
        ):
            keep = own.shape[1]
            to = 0 if side else width * full
            stage[side, to : to + keep] = own[side]
            for k in range(width):
                at = base + k * narrow
                to = k * full + 4 + (keep if side else 0)
                stage[side, to : to + narrow] = halo[side, at : at + narrow]
        for r in range(6):
            for h in range(2):
                x33[side, r, :, h * 128 : (h + 1) * 128] = e33[side, h, r * W3 : (r + 1) * W3].astype(BF16)
        fresh, kept = (2, 0) if side else (0, 4)
        x32[side, kept : kept + 2] = y32[side]
        x31[side, kept : kept + 2] = y31[side]
        fresh, kept = (2, 0) if side else (0, 8)
        g22[side, kept : kept + 2] = y22[side]
        g21[side, kept : kept + 2] = y21[side]

    def pick_both(x, count):
        return lambda dy: x[:, 2 - dy : 2 - dy + count].reshape(2 * count * x.shape[2], x.shape[3])

    for x, kernel, stage, nxt in ((x33, k33, e32, x32), (x32, k32, e31, x31)):
        value = conv(pick_both(x, 4), kernel)
        for side in range(2):
            for h in range(2):
                part = value[side * 4 * W3 : (side + 1) * 4 * W3, h * 128 : (h + 1) * 128]
                part = jnp.where(stage[side, h] > 0, part, 0.0).astype(BF16).reshape(4, W3, 128)
                nxt[side, 2 * side : 2 * side + 4, :, h * 128 : (h + 1) * 128] = part
    value = conv(pick_both(x31, 4), k31)
    for side in range(2):
        for k in range(4):
            at = (side * 4 + k) * W3
            spread(value[at : at + W3], ea[side, k * W3 : (k + 1) * W3], u2.at[side], k)
        for r in range(8):
            at = slice(r * W2, (r + 1) * W2)
            arriving = u2[side, r * WU + LEAD : r * WU + LEAD + W2] + ei[side, at]
            g22[side, 2 * side + r] = jnp.where(e22[side, at] > 0, arriving, 0.0).astype(BF16)

    @pl.loop(0, 2)
    def _(side):
        value = conv(block(g22.at[side], 0, 8), k22)
        value = jnp.where(e21[side] > 0, value, 0.0).astype(BF16)
        g21[side, pl.ds(2 * side, 8)] = value.reshape(8, W2, 128)

    @pl.loop(0, 2)
    def _(side):
        value = conv(block(g21.at[side], 0, 8), k21d)
        for k in range(8):
            p1[side, k * WP : k * WP + W2] = value[k * W2 : (k + 1) * W2]

    emit(a1, ((0, 8, p1.at[0], obuf.at[0]), (tall - 8, 8, p1.at[1], obuf.at[1])), o1)
    moves = [
        pltpu.make_async_copy(obuf.at[0], result.at[0:16], sem.at[0]),
        pltpu.make_async_copy(obuf.at[1], result.at[2 * tall - 16 : 2 * tall], sem.at[1]),
    ]
    for move in moves:
        move.start()
    for move in moves:
        move.wait()


def whole(array):
    zeros = (0,) * len(array.shape)
    return pl.BlockSpec(array.shape, lambda i: zeros)


STORED = pl.BlockSpec(memory_space=pltpu.MemorySpace.HBM)


def call(body, args, outs, scratch=(), specs=None, out_specs=None, aliases=None, cost=0, limit=8):
    shapes = [jax.ShapeDtypeStruct(s, d) for s, d in outs]
    return pl.pallas_call(
        body,
        grid=(1,),
        in_specs=specs or [whole(a) for a in args],
        out_specs=out_specs or [whole(s) for s in shapes],
        out_shape=shapes,
        input_output_aliases=aliases or {},
        scratch_shapes=[pltpu.VMEM(*s) if isinstance(s, tuple) else s for s in scratch],
        cost_estimate=pl.CostEstimate(flops=cost, bytes_accessed=4000000, transcendentals=0),
        compiler_params=pltpu.CompilerParams(vmem_limit_bytes=limit << 20),
    )(*args)


def swap(first, last, axis):
    count = lax.axis_size(axis)
    from_before = lax.ppermute(last, axis, [(i, i + 1) for i in range(count - 1)])
    from_after = lax.ppermute(first, axis, [(i + 1, i) for i in range(count - 1)])
    return from_before, from_after


def shards(m21, m22, m31, m32, m33, t22, t33, a1, a2, w2, w3, k21, k22, k31, k32, k33):
    rows, cols, ch3 = m33.shape
    tall, wide, ch2 = m22.shape
    w2 = w2.reshape(1, ch2)
    w3 = w3.reshape(1, ch3)
    args = tuple(
        pltpu.with_memory_space_constraint(x, pltpu.MemorySpace.HBM)
        for x in (m33, t33, m32, m31, m22, t22, m21, a2, w2, w3)
    )
    seeds, left, right = call(
        pack_cols, args,
        [((rows, cols, ch3), BF16), ((COL_TOTAL, 128), BF16), ((COL_TOTAL, 128), BF16)],
        scratch=[
            ((rows, cols, ch3), BF16), ((rows, cols, ch3), BF16), ((2, rows, 8, ch3), BF16),
            ((2, rows, 8, ch3), BF16), ((2, tall, 8, ch2), BF16), ((2, tall, 8, ch2), BF16),
            ((2, tall, 8, ch2), BF16), ((2, rows, 128), a2.dtype), (w2.shape, F32), (w3.shape, F32),
            ((12, rows * 8, 128), F32), ((6, tall * 8, 128), F32), ((2, COL_TOTAL, 128), F32),
            pltpu.SemaphoreType.DMA((18,)),
        ],
        specs=[STORED] * 10, cost=10**9, limit=LIM[0],
    )
    fl, fr = swap(left, right, "col")
    i22, k21d = call(
        own_inject, (m22, t22, w2, k21.T),
        [((tall, wide, ch2), F32), ((k21.shape[0], 9 * 128), BF16)], cost=10**9, limit=LIM[1],
    )
    up, down = call(
        pack_rows, (seeds, m32, m31, m22, i22, m21, a2, fl, fr),
        [((ROW_TOTAL, 128), BF16), ((ROW_TOTAL, 128), BF16)],
        scratch=[((COL_TOTAL, 128), F32), ((COL_TOTAL, 128), F32), ((2, ROW_TOTAL, 128), F32)],
        cost=10**9, limit=LIM[2],
    )
    above, below = swap(up, down, "row")
    area3, area2 = rows * W3, tall * W2
    edges = [
        ((2, 2, 2 * W3, 128), F32), ((2, 2, W3, 128), F32), ((2, 2, 2 * W3, 128), F32), ((2, 3 * W3, 128), F32),
        ((2, 6 * W2, 128), F32), ((2, 6 * W2, 128), F32), ((2, 7 * W2, 128), F32),
        ((2, 2, W3, ch3), BF16), ((2, 2, W3, ch3), BF16), ((2, 2, W2, ch2), BF16), ((2, 2, W2, ch2), BF16),
    ]
    shape = (2 * tall, 2 * wide * 64)
    partial, *state = call(
        inner,
        (seeds, m32, m31, m22, i22, m21, a2, a1, fl, fr, k33, k32, k31, k22, k21d),
        [(shape, BF16)] + edges,
        out_specs=[STORED] + [whole(jax.ShapeDtypeStruct(s, d)) for s, d in edges],
        scratch=[
            ((2, area3, 128), F32), ((2, area3, 128), F32), ((2, area3, 128), F32), ((area3, 128), F32),
            ((area2, 128), F32), ((area2, 128), F32), ((area2, 128), F32),
            ((rows, W3, ch3), BF16), ((rows - 2, W3, ch3), BF16), ((rows - 4, W3, ch3), BF16),
            (((tall - 12) * WU, 128), F32), ((tall - 12, W2, ch2), BF16), ((tall - 14, W2, ch2), BF16),
            (((tall - 16) * WP, 128), F32), ((8, 2 * tall, 128), F32), ((2 * tall - 32, shape[1]), BF16),
            pltpu.SemaphoreType.DMA(()),
        ],
        cost=10**10, limit=LIM[3],
    )
    args = (*state, above, below, a1, k33, k32, k31, k22, k21d)
    (result,) = call(
        outer, (*args, partial), [(shape, BF16)],
        specs=[whole(a) for a in args] + [STORED], out_specs=[STORED], aliases={len(args): 0},
        scratch=[
            ((2, ROW_TOTAL, 128), F32),
            ((2, 2, 6 * W3, 128), F32), ((2, 2, 4 * W3, 128), F32), ((2, 2, 4 * W3, 128), F32),
            ((2, 4 * W3, 128), F32), ((2, 8 * W2, 128), F32), ((2, 8 * W2, 128), F32), ((2, 8 * W2, 128), F32),
            ((2, 6, W3, ch3), BF16), ((2, 6, W3, ch3), BF16), ((2, 6, W3, ch3), BF16),
            ((2, 8 * WU, 128), F32), ((2, 10, W2, ch2), BF16), ((2, 10, W2, ch2), BF16),
            ((2, 8 * WP, 128), F32), ((8, 16, 128), F32), ((2, 16, shape[1]), BF16),
            pltpu.SemaphoreType.DMA((2,)),
        ],
        cost=10**9, limit=LIM[4],
    )
    return result


def solution(mesh):
    in_specs = (P("row", "col", None),) * 7 + (P("row", "col"),) * 2 + (P(),) * 7
    return jax.shard_map(
        shards, mesh=mesh, in_specs=in_specs, out_specs=P("row", "col"), check_vma=False
    )
```

```python
import jax
import jax.numpy as jnp
from jax import lax
from jax.experimental import pallas as pl
from jax.experimental.pallas import tpu as pltpu
from jax.sharding import PartitionSpec as P

EPSILON = 1e-06
F32 = jnp.float32
BF16 = jnp.bfloat16

COL_SEED, COL_M32, COL_M31, COL_M22, COL_I22, COL_M21, COL_A2, COL_TOTAL = (
    0, 128, 224, 288, 352, 416, 448, 464)
ROW_SEED, ROW_M32, ROW_M31, ROW_A2, ROW_M22, ROW_I22, ROW_M21, ROW_TOTAL = (
    0, 320, 560, 720, 760, 904, 1048, 1120)
T3, T2 = 40, 72
W3, W2, WU, WP = 48, 80, 96, 88
LEAD = 8
LIM = (8, 10, 8, 26, 26)
STEP2, STEP3 = 16, 8
GROUP = 8
SPLIT3, SPLIT31, SPLIT2 = 2, 2, 2
SIDES = 2


def inject(preact, target, weight):
    count = preact.shape[-1]
    feature = jnp.maximum(preact.astype(F32), 0.0)
    wanted = jnp.maximum(target.astype(F32), 0.0)
    scale = lax.rsqrt(jnp.sum(feature * feature, axis=-1, keepdims=True) * (1.0 / count) + EPSILON)
    other = lax.rsqrt(jnp.sum(wanted * wanted, axis=-1, keepdims=True) * (1.0 / count) + EPSILON)
    scaled = feature * scale
    excess = (2.0 * weight) * (scaled - wanted * other)
    mean = jnp.sum(excess * scaled, axis=-1, keepdims=True) * (1.0 / count)
    return (excess - scaled * mean) * scale


def pack_cols(hm33, ht33, hm32, hm31, hm22, ht22, hm21, ha2, hw2, hw3, left, right,
              m33, t33, m32, m31, m22, t22, m21, a2, w2, w3, st3, st2, flat, sems):
    rows, cols, ch = hm33.shape
    tall, wide, _ = hm22.shape
    moves = []
    for source, target in (
        (hm33.at[:, 0:8], m33.at[0]), (hm33.at[:, cols - 8 : cols], m33.at[1]),
        (ht33.at[:, 0:8], t33.at[0]), (ht33.at[:, cols - 8 : cols], t33.at[1]),
        (hm22.at[:, 0:8], m22.at[0]), (hm22.at[:, wide - 8 : wide], m22.at[1]),
        (ht22.at[:, 0:8], t22.at[0]), (ht22.at[:, wide - 8 : wide], t22.at[1]),
        (hm32.at[:, 0:8], m32.at[0]), (hm32.at[:, cols - 8 : cols], m32.at[1]),
        (hm31.at[:, 0:8], m31.at[0]), (hm31.at[:, cols - 8 : cols], m31.at[1]),
        (hm21.at[:, 0:8], m21.at[0]), (hm21.at[:, wide - 8 : wide], m21.at[1]),
        (ha2.at[:, 0:128], a2.at[0]), (ha2.at[:, (cols - 1) * 128 : cols * 128], a2.at[1]),
        (hw2, w2), (hw3, w3),
    ):
        moves.append(pltpu.make_async_copy(source, target, sems.at[len(moves)]))
        moves[-1].start()
    for move in moves:
        move.wait()
    for side, out in enumerate((left, right)):
        p = m33[side].reshape(rows * 8, ch)
        seeds = inject(p, t33[side].reshape(rows * 8, ch), w3[...])
        seeds = jnp.where(p.astype(F32) > 0, seeds, 0.0).reshape(rows, 8, ch)
        for g, (base, width) in enumerate(((COL_SEED, 4), (COL_M32, 3), (COL_M31, 2))):
            pick = 8 - width if side else 0
            for h in range(2):
                lanes = slice(h * 128, (h + 1) * 128)
                own = (seeds[:, :, lanes], m32[side, :, :, lanes], m31[side, :, :, lanes])[g]
                stage = st3.at[(g * 2 + side) * 2 + h]
                stage[...] = own.astype(F32).reshape(rows * 8, 128)
                for c in range(width):
                    to = base + (c * 2 + h) * rows
                    flat[side, to : to + rows] = stage[pl.ds(pick + c, rows, stride=8), :]
        p = m22[side].reshape(tall * 8, 128)
        groups = (
            (COL_M22, 2, p.astype(F32)),
            (COL_I22, 2, inject(p, t22[side].reshape(tall * 8, 128), w2[...])),
            (COL_M21, 1, m21[side].astype(F32).reshape(tall * 8, 128)),
        )
        for g, (base, width, own) in enumerate(groups):
            pick = 8 - width if side else 0
            stage = st2.at[g * 2 + side]
            stage[...] = own
            for c in range(width):
                to = base + c * tall
                flat[side, to : to + tall] = stage[pl.ds(pick + c, tall, stride=8), :]
        flat[side, COL_A2 : COL_A2 + rows] = a2[side].astype(F32)
        out[...] = flat[side].astype(BF16)

def own_inject(m22, t22, m33, t33, w2, w3, k21, k22, i22, seeds, k21p, k22p):
    tall, wide, _ = m22.shape
    rows, cols, ch = m33.shape

    @pl.loop(0, tall // STEP2)
    def _(i):
        at = pl.ds(i * STEP2, STEP2)
        p = m22[at].reshape(STEP2 * wide, 128)
        i22[at] = inject(p, t22[at].reshape(STEP2 * wide, 128), w2[...]).reshape(STEP2, wide, 128)

    @pl.loop(0, rows // STEP3)
    def _(i):
        at = pl.ds(i * STEP3, STEP3)
        p = m33[at].reshape(STEP3 * cols, ch)
        value = inject(p, t33[at].reshape(STEP3 * cols, ch), w3[...])
        seeds[at] = jnp.where(p.astype(F32) > 0, value, 0.0).astype(BF16).reshape(STEP3, cols, ch)

    half = k21.shape[0] // 9
    span = k22.shape[1] // 3
    for dy in range(3):
        taps = [k21[(3 * dy + dx) * half : (3 * dy + dx + 1) * half].astype(F32) for dx in (0, 2, 1, 1)]
        rows_of = slice(dy * 128, (dy + 1) * 128)
        k21p[rows_of, 0:128] = jnp.concatenate(taps[:2], axis=0).T.astype(BF16)
        k21p[rows_of, 128:256] = jnp.concatenate(taps[2:], axis=0).T.astype(BF16)
        k22p[rows_of] = k22[:, dy * span : (dy + 1) * span]


def pack_rows(seeds, m32, m31, m22, i22, m21, a2, fl, fr, up, down, side_l, side_r, flat):
    rows, cols, _ = seeds.shape
    tall, wide, _ = m22.shape
    side_l[...] = fl[...].astype(F32)
    side_r[...] = fr[...].astype(F32)
    for side, out in enumerate((up, down)):
        for source, base, col_base, width in (
            (seeds, ROW_SEED, COL_SEED, 4), (m32, ROW_M32, COL_M32, 3), (m31, ROW_M31, COL_M31, 2),
        ):
            r0 = rows - width if side else 0
            for h in range(2):
                for k in range(width):
                    to = base + (k * 2 + h) * T3 + 4
                    flat[side, to : to + cols] = source[r0 + k, :, h * 128 : (h + 1) * 128].astype(F32)
                for c in range(width):
                    at = col_base + (c * 2 + h) * rows + r0
                    to = base + h * T3
                    flat.at[side][pl.ds(to + 4 - width + c, width, stride=2 * T3), :] = side_l[at : at + width]
                    flat.at[side][pl.ds(to + 4 + cols + c, width, stride=2 * T3), :] = side_r[at : at + width]
        for source, base, col_base, width in (
            (m22, ROW_M22, COL_M22, 2), (i22, ROW_I22, COL_I22, 2), (m21, ROW_M21, COL_M21, 1),
        ):
            r0 = tall - width if side else 0
            for k in range(width):
                to = base + k * T2 + 4
                flat[side, to : to + wide] = source[r0 + k].astype(F32)
                for c in range(width):
                    at = col_base + c * tall + r0 + k
                    flat[side, to - width + c : to - width + c + 1] = side_l[at : at + 1]
                    flat[side, to + wide + c : to + wide + c + 1] = side_r[at : at + 1]
        r0 = rows - 1 if side else 0
        line = a2[r0 : r0 + 1, :].astype(F32)
        to = ROW_A2 + 4
        for c in range(cols):
            flat[side, to + c : to + c + 1] = line[:, c * 128 : (c + 1) * 128]
        at = COL_A2 + r0
        flat[side, to - 1 : to] = side_l[at : at + 1]
        flat[side, to + cols : to + cols + 1] = side_r[at : at + 1]
        out[...] = flat[side].astype(BF16)


def conv(pick, kernel):
    span = kernel.shape[1] // 3
    total = None
    for dy in range(3):
        term = jnp.dot(pick(dy), kernel[:, dy * span : (dy + 1) * span], preferred_element_type=F32)
        total = term if total is None else total + term
    return shifted(total)


def shifted(total):
    n = total.shape[1] // 3
    before = pltpu.roll(total[:, :n], total.shape[0] - 1, 0)
    after = pltpu.roll(total[:, 2 * n :], 1, 0)
    return before + total[:, n : 2 * n] + after


def paired(x, kernel, row, count):
    size = count * x.shape[1]
    upper = x[pl.ds(row + 2, count)].reshape(size, 256)
    lower = x[pl.ds(row, count), :, 0:128].reshape(size, 128)
    return jnp.dot(upper, kernel[0:256], preferred_element_type=F32) + jnp.dot(
        lower, kernel[256:384], preferred_element_type=F32
    )


def doubled(total):
    size = total.shape[0]
    sides = total[:, 0:128]
    low = lax.broadcasted_iota(jnp.int32, sides.shape, 1) < 64
    sides = jnp.where(low, pltpu.roll(sides, size - 1, 0), pltpu.roll(sides, 1, 0))
    return total[:, 128:256] + sides + pltpu.roll(sides, 64, 1)


def store_pair(x, row, count, value):
    x[pl.ds(row, count), :, 0:128] = value
    x[pl.ds(row + 1, count), :, 128:256] = value


def block(x, row, count):
    def pick(dy):
        return x[pl.ds(row + 2 - dy, count)].reshape(count * x.shape[1], x.shape[2])

    return pick


def spread(part, where, u2, row):
    for a in range(2):
        for b in range(2):
            to = (2 * row + a) * WU + b
            u2[pl.ds(to, W3, stride=2), :] = jnp.where(where == 2.0 * a + b, part, 0.0)


def emit(a1, pieces, o1, result, sems):
    tiles = a1.shape[1] // 128
    group = GROUP

    moves = []
    for i in range(tiles // group):
        for part, (first, count, p1, out, top) in enumerate(pieces):
            high = lax.broadcasted_iota(jnp.int32, (count, 128), 1) >= 64
            shift = jnp.where(high, 1, 0)
            for j in range(group):
                t = i * group + j
                where = a1[first : first + count, t * 128 : (t + 1) * 128]
                turned = pltpu.roll(where, 64, 1)
                for odd in range(2):
                    own = (jnp.where(high, where, turned) if odd else jnp.where(high, turned, where)) - shift
                    value = p1[pl.ds(LEAD + 2 * t + odd, count, stride=WP), :]
                    slot = o1.at[(part * group + j) * 2 + odd]
                    for a in range(2):
                        slot[pl.ds(a, count, stride=2), :] = jnp.where(own == 2 * a, value, 0.0)
                    to = (2 * t + odd) * 128
                    out[:, to : to + 128] = slot[0 : 2 * count].astype(BF16)
            lanes = slice(2 * i * group * 128, 2 * (i + 1) * group * 128)
            moves.append(
                pltpu.make_async_copy(
                    out.at[:, lanes], result.at[top : top + 2 * count, lanes], sems.at[len(moves)]
                )
            )
            moves[-1].start()
    return moves


def inner(seeds, m32, m31, m22, i22, m21, a2, a1, fl, fr, k33, k32, k31, k22, k21d,
          result, t33, t32, t31, ta, t22, ti, t21, y32, y31, y22, y21,
          e33, e32, e31, ea, e22, ei, e21, x33, x32, x31, u2, g22, g21, p1, o1, obuf, sem):
    rows, cols, _ = seeds.shape
    tall, wide, _ = m22.shape
    for source, stage, col_base, width in (
        (seeds, e33, COL_SEED, 4), (m32, e32, COL_M32, 3), (m31, e31, COL_M31, 2),
    ):

        @pl.loop(0, rows // 4)
        def _(i):
            for j in range(4):
                r = i * 4 + j
                to = pl.multiple_of(r * W3 + LEAD, 8)
                for h in range(2):
                    stage[h, pl.ds(to, cols)] = source[r, :, h * 128 : (h + 1) * 128].astype(F32)

        for h in range(2):
            for c in range(width):
                at = col_base + (c * 2 + h) * rows
                stage.at[h][pl.ds(LEAD - width + c, rows, stride=W3), :] = fl[at : at + rows].astype(F32)
                stage.at[h][pl.ds(LEAD + cols + c, rows, stride=W3), :] = fr[at : at + rows].astype(F32)
    for source, stage, col_base, width in (
        (m22, e22, COL_M22, 2), (i22, ei, COL_I22, 2), (m21, e21, COL_M21, 1),
    ):

        @pl.loop(0, tall // 4)
        def _(i):
            for j in range(4):
                r = i * 4 + j
                stage[pl.ds(pl.multiple_of(r * W2 + LEAD, 8), wide)] = source[r].astype(F32)

        for c in range(width):
            at = col_base + c * tall
            stage[pl.ds(LEAD - width + c, tall, stride=W2), :] = fl[at : at + tall].astype(F32)
            stage[pl.ds(LEAD + wide + c, tall, stride=W2), :] = fr[at : at + tall].astype(F32)
    for c in range(cols):
        ea[pl.ds(LEAD + c, rows, stride=W3), :] = a2[:, c * 128 : (c + 1) * 128].astype(F32)
    ea[pl.ds(LEAD - 1, rows, stride=W3), :] = fl[COL_A2 : COL_A2 + rows].astype(F32)
    ea[pl.ds(LEAD + cols, rows, stride=W3), :] = fr[COL_A2 : COL_A2 + rows].astype(F32)

    @pl.loop(0, rows // 2)
    def _(i):
        for j in range(2):
            at = pl.ds(pl.multiple_of((i * 2 + j) * W3, W3), W3)
            for h in range(2):
                x33[i * 2 + j, :, h * 128 : (h + 1) * 128] = e33[h, at].astype(BF16)

    for x, kernel, stage, nxt, skip in ((x33, k33, e32, x32, 1), (x32, k32, e31, x31, 2)):
        count = nxt.shape[0] // SPLIT3

        @pl.loop(0, SPLIT3)
        def _(i):
            row = i * count
            value = conv(block(x, row, count), kernel)
            at = pl.ds(pl.multiple_of((row + skip) * W3, W3), count * W3)
            for h in range(2):
                part = jnp.where(stage[h, at] > 0, value[:, h * 128 : (h + 1) * 128], 0.0)
                nxt[pl.ds(row, count), :, h * 128 : (h + 1) * 128] = part.astype(BF16).reshape(
                    count, W3, 128
                )

    count = (rows - 6) // SPLIT31

    @pl.loop(0, SPLIT31)
    def _(i):
        row = i * count
        value = conv(block(x31, row, count), k31)
        for k in range(count):
            where = ea[pl.ds(pl.multiple_of((row + k + 3) * W3, W3), W3)]
            spread(value[k * W3 : (k + 1) * W3], where, u2, row + k)

    @pl.loop(0, (tall - 12) // 2)
    def _(i):
        for j in range(2):
            r = i * 2 + j
            at = pl.ds(pl.multiple_of((r + 6) * W2, W2), W2)
            arriving = u2[pl.ds(pl.multiple_of(r * WU + LEAD, 8), W2)] + ei[at]
            store_pair(g22, r, 1, jnp.where(e22[at] > 0, arriving, 0.0).astype(BF16).reshape(1, W2, 128))

    count = (tall - 14) // SPLIT2

    @pl.loop(0, SPLIT2)
    def _(i):
        row = i * count
        value = shifted(paired(g22, k22, row, count))
        at = pl.ds(pl.multiple_of((row + 7) * W2, W2), count * W2)
        value = jnp.where(e21[at] > 0, value, 0.0)
        store_pair(g21, row, count, value.astype(BF16).reshape(count, W2, 128))

    half = (tall - 16) // SPLIT2

    @pl.loop(0, SPLIT2)
    def _(i):
        row = i * half
        value = doubled(paired(g21, k21d, row, half))
        for k in range(half):
            p1[pl.ds(pl.multiple_of((row + k) * WP, 8), W2)] = value[k * W2 : (k + 1) * W2]

    moves = emit(a1, ((8, tall - 16, p1, obuf, 16),), o1, result, sem)
    for side in range(2):
        for target, stage, count, width in (
            (t33, e33, 2, W3), (t32, e32, 1, W3), (t31, e31, 2, W3),
        ):
            r0 = (rows - count) * side
            target[side] = stage[:, r0 * width : (r0 + count) * width]
        for target, stage, count, width, total in (
            (ta, ea, 3, W3, rows), (t22, e22, 6, W2, tall), (ti, ei, 6, W2, tall), (t21, e21, 7, W2, tall),
        ):
            r0 = (total - count) * side
            target[side] = stage[r0 * width : (r0 + count) * width]
        for target, source, count in (
            (y32, x32, rows - 2), (y31, x31, rows - 4), (y22, g22, tall - 12), (y21, g21, tall - 14),
        ):
            r0 = (count - 2) * side
            target[side] = source[r0 : r0 + 2, :, 0 : target.shape[3]]
    for move in moves:
        move.wait()


def outer(t33, t32, t31, ta, t22, ti, t21, y32, y31, y22, y21, above, below, a1,
          k33, k32, k31, k22, k21d, partial, result,
          halo, e33, e32, e31, ea, e22, ei, e21, x33, x32, x31, u2, g22, g21, p1, o1, obuf, sem):
    del partial
    tall = result.shape[0] // 2
    halo[0] = above[...].astype(F32)
    halo[1] = below[...].astype(F32)
    for side in range(2):
        for own, stage, base, width in (
            (t33, e33, ROW_SEED, 4), (t32, e32, ROW_M32, 3), (t31, e31, ROW_M31, 2),
        ):
            keep = own.shape[2]
            for h in range(2):
                to = 0 if side else width * W3
                stage[side, h, to : to + keep] = own[side, h]
                for k in range(width):
                    at = base + (k * 2 + h) * T3
                    to = k * W3 + 4 + (keep if side else 0)
                    stage[side, h, to : to + T3] = halo[side, at : at + T3]
        for own, stage, base, width, narrow, full in (
            (ta, ea, ROW_A2, 1, T3, W3), (t22, e22, ROW_M22, 2, T2, W2),
            (ti, ei, ROW_I22, 2, T2, W2), (t21, e21, ROW_M21, 1, T2, W2),
        ):
            keep = own.shape[1]
            to = 0 if side else width * full
            stage[side, to : to + keep] = own[side]
            for k in range(width):
                at = base + k * narrow
                to = k * full + 4 + (keep if side else 0)
                stage[side, to : to + narrow] = halo[side, at : at + narrow]
        for r in range(6):
            for h in range(2):
                x33[side, r, :, h * 128 : (h + 1) * 128] = e33[side, h, r * W3 : (r + 1) * W3].astype(BF16)
        fresh, kept = (2, 0) if side else (0, 4)
        x32[side, kept : kept + 2] = y32[side]
        x31[side, kept : kept + 2] = y31[side]
        fresh, kept = (2, 0) if side else (0, 8)
        store_pair(g22.at[side], kept, 2, y22[side])
        store_pair(g21.at[side], kept, 2, y21[side])

    def pick_both(x, count):
        return lambda dy: x[:, 2 - dy : 2 - dy + count].reshape(2 * count * x.shape[2], x.shape[3])

    for x, kernel, stage, nxt in ((x33, k33, e32, x32), (x32, k32, e31, x31)):
        value = conv(pick_both(x, 4), kernel)
        for side in range(2):
            for h in range(2):
                part = value[side * 4 * W3 : (side + 1) * 4 * W3, h * 128 : (h + 1) * 128]
                part = jnp.where(stage[side, h] > 0, part, 0.0).astype(BF16).reshape(4, W3, 128)
                nxt[side, 2 * side : 2 * side + 4, :, h * 128 : (h + 1) * 128] = part
    value = conv(pick_both(x31, 4), k31)
    for side in range(2):
        for k in range(4):
            at = (side * 4 + k) * W3
            spread(value[at : at + W3], ea[side, k * W3 : (k + 1) * W3], u2.at[side], k)
        for r in range(8):
            at = slice(r * W2, (r + 1) * W2)
            arriving = u2[side, r * WU + LEAD : r * WU + LEAD + W2] + ei[side, at]
            arriving = jnp.where(e22[side, at] > 0, arriving, 0.0).astype(BF16)
            store_pair(g22.at[side], 2 * side + r, 1, arriving.reshape(1, W2, 128))

    def second(side):
        value = shifted(paired(g22.at[side], k22, 0, 8))
        value = jnp.where(e21[side] > 0, value, 0.0).astype(BF16)
        store_pair(g21.at[side], 2 * side, 8, value.reshape(8, W2, 128))

    def first(side):
        value = doubled(paired(g21.at[side], k21d, 0, 8))
        for k in range(8):
            p1[side, k * WP : k * WP + W2] = value[k * W2 : (k + 1) * W2]

    for step in (second, first):
        if SIDES == 1:
            pl.loop(0, 2)(step)
        else:
            for side in range(2):
                step(side)

    moves = emit(
        a1,
        ((0, 8, p1.at[0], obuf.at[0], 0), (tall - 8, 8, p1.at[1], obuf.at[1], 2 * tall - 16)),
        o1, result, sem,
    )
    for move in moves:
        move.wait()


def whole(array):
    zeros = (0,) * len(array.shape)
    return pl.BlockSpec(array.shape, lambda i: zeros)


STORED = pl.BlockSpec(memory_space=pltpu.MemorySpace.HBM)


def call(body, args, outs, scratch=(), specs=None, out_specs=None, aliases=None, cost=0, limit=8):
    shapes = [jax.ShapeDtypeStruct(s, d) for s, d in outs]
    return pl.pallas_call(
        body,
        grid=(1,),
        in_specs=specs or [whole(a) for a in args],
        out_specs=out_specs or [whole(s) for s in shapes],
        out_shape=shapes,
        input_output_aliases=aliases or {},
        scratch_shapes=[pltpu.VMEM(*s) if isinstance(s, tuple) else s for s in scratch],
        cost_estimate=pl.CostEstimate(flops=cost, bytes_accessed=4000000, transcendentals=0),
        compiler_params=pltpu.CompilerParams(vmem_limit_bytes=limit << 20),
    )(*args)


def swap(first, last, axis):
    count = lax.axis_size(axis)
    from_before = lax.ppermute(last, axis, [(i, i + 1) for i in range(count - 1)])
    from_after = lax.ppermute(first, axis, [(i + 1, i) for i in range(count - 1)])
    return from_before, from_after


def shards(m21, m22, m31, m32, m33, t22, t33, a1, a2, w2, w3, k21, k22, k31, k32, k33):
    rows, cols, ch3 = m33.shape
    tall, wide, ch2 = m22.shape
    w2 = w2.reshape(1, ch2)
    w3 = w3.reshape(1, ch3)
    args = tuple(
        pltpu.with_memory_space_constraint(x, pltpu.MemorySpace.HBM)
        for x in (m33, t33, m32, m31, m22, t22, m21, a2, w2, w3)
    )
    left, right = call(
        pack_cols, args,
        [((COL_TOTAL, 128), BF16), ((COL_TOTAL, 128), BF16)],
        scratch=[
            ((2, rows, 8, ch3), BF16), ((2, rows, 8, ch3), BF16), ((2, rows, 8, ch3), BF16),
            ((2, rows, 8, ch3), BF16), ((2, tall, 8, ch2), BF16), ((2, tall, 8, ch2), BF16),
            ((2, tall, 8, ch2), BF16), ((2, rows, 128), a2.dtype), (w2.shape, F32), (w3.shape, F32),
            ((12, rows * 8, 128), F32), ((6, tall * 8, 128), F32), ((2, COL_TOTAL, 128), F32),
            pltpu.SemaphoreType.DMA((18,)),
        ],
        specs=[STORED] * 10, cost=10**9, limit=LIM[0],
    )
    fl, fr = swap(left, right, "col")
    i22, seeds, k21d, k22 = call(
        own_inject, (m22, t22, m33, t33, w2, w3, k21.T, k22),
        [((tall, wide, ch2), F32), ((rows, cols, ch3), BF16), ((3 * ch2, 256), BF16), ((3 * ch2, 384), BF16)],
        cost=10**9, limit=LIM[1],
    )
    up, down = call(
        pack_rows, (seeds, m32, m31, m22, i22, m21, a2, fl, fr),
        [((ROW_TOTAL, 128), BF16), ((ROW_TOTAL, 128), BF16)],
        scratch=[((COL_TOTAL, 128), F32), ((COL_TOTAL, 128), F32), ((2, ROW_TOTAL, 128), F32)],
        cost=10**9, limit=LIM[2],
    )
    above, below = swap(up, down, "row")
    area3, area2 = rows * W3, tall * W2
    edges = [
        ((2, 2, 2 * W3, 128), F32), ((2, 2, W3, 128), F32), ((2, 2, 2 * W3, 128), F32), ((2, 3 * W3, 128), F32),
        ((2, 6 * W2, 128), F32), ((2, 6 * W2, 128), F32), ((2, 7 * W2, 128), F32),
        ((2, 2, W3, ch3), BF16), ((2, 2, W3, ch3), BF16), ((2, 2, W2, ch2), BF16), ((2, 2, W2, ch2), BF16),
    ]
    shape = (2 * tall, 2 * wide * 64)
    partial, *state = call(
        inner,
        (seeds, m32, m31, m22, i22, m21, a2, a1, fl, fr, k33, k32, k31, k22, k21d),
        [(shape, BF16)] + edges,
        out_specs=[STORED] + [whole(jax.ShapeDtypeStruct(s, d)) for s, d in edges],
        scratch=[
            ((2, area3, 128), F32), ((2, area3, 128), F32), ((2, area3, 128), F32), ((area3, 128), F32),
            ((area2, 128), F32), ((area2, 128), F32), ((area2, 128), F32),
            ((rows, W3, ch3), BF16), ((rows - 2, W3, ch3), BF16), ((rows - 4, W3, ch3), BF16),
            (((tall - 12) * WU, 128), F32), ((tall - 11, W2, 256), BF16), ((tall - 13, W2, 256), BF16),
            (((tall - 16) * WP, 128), F32), ((2 * GROUP, 2 * tall - 32, 128), F32), ((2 * tall - 32, shape[1]), BF16),
            pltpu.SemaphoreType.DMA((wide // 2 // GROUP,)),
        ],
        cost=10**10, limit=LIM[3],
    )
    args = (*state, above, below, a1, k33, k32, k31, k22, k21d)
    (result,) = call(
        outer, (*args, partial), [(shape, BF16)],
        specs=[whole(a) for a in args] + [STORED], out_specs=[STORED], aliases={len(args): 0},
        scratch=[
            ((2, ROW_TOTAL, 128), F32),
            ((2, 2, 6 * W3, 128), F32), ((2, 2, 4 * W3, 128), F32), ((2, 2, 4 * W3, 128), F32),
            ((2, 4 * W3, 128), F32), ((2, 8 * W2, 128), F32), ((2, 8 * W2, 128), F32), ((2, 8 * W2, 128), F32),
            ((2, 6, W3, ch3), BF16), ((2, 6, W3, ch3), BF16), ((2, 6, W3, ch3), BF16),
            ((2, 8 * WU, 128), F32), ((2, 11, W2, 256), BF16), ((2, 11, W2, 256), BF16),
            ((2, 8 * WP, 128), F32), ((4 * GROUP, 16, 128), F32), ((2, 16, shape[1]), BF16),
            pltpu.SemaphoreType.DMA((2 * (wide // 2 // GROUP),)),
        ],
        cost=10**9, limit=LIM[4],
    )
    return result


def solution(mesh):
    in_specs = (P("row", "col", None),) * 7 + (P("row", "col"),) * 2 + (P(),) * 7
    return jax.shard_map(
        shards, mesh=mesh, in_specs=in_specs, out_specs=P("row", "col"), check_vma=False
    )
```

```python
import jax
import jax.numpy as jnp
from jax import lax
from jax.experimental import pallas as pl
from jax.experimental.pallas import tpu as pltpu
from jax.sharding import PartitionSpec as P

EPSILON = 1e-06
F32 = jnp.float32
BF16 = jnp.bfloat16

COL_SEED, COL_M32, COL_M31, COL_M22, COL_I22, COL_M21, COL_A2, COL_TOTAL = (
    0, 128, 224, 288, 352, 416, 448, 464)
ROW_SEED, ROW_M32, ROW_M31, ROW_A2, ROW_M22, ROW_I22, ROW_M21, ROW_TOTAL = (
    0, 320, 560, 720, 760, 904, 1048, 1120)
T3, T2 = 40, 72
W3, W2, WU, WP = 48, 80, 96, 88
LEAD = 8
LIM = (8, 10, 8, 26, 26)
STEP2, STEP3 = 16, 8
GROUP = 8
FLAGS = [None] * 5
UNROLL = (1, 1, 1, 1)
PERSIDE = 1
SPLIT3, SPLIT31, SPLIT2 = 2, 2, 2
SIDES = 2


def inject(preact, target, weight):
    count = preact.shape[-1]
    feature = jnp.maximum(preact.astype(F32), 0.0)
    wanted = jnp.maximum(target.astype(F32), 0.0)
    scale = lax.rsqrt(jnp.sum(feature * feature, axis=-1, keepdims=True) * (1.0 / count) + EPSILON)
    other = lax.rsqrt(jnp.sum(wanted * wanted, axis=-1, keepdims=True) * (1.0 / count) + EPSILON)
    scaled = feature * scale
    excess = (2.0 * weight) * (scaled - wanted * other)
    mean = jnp.sum(excess * scaled, axis=-1, keepdims=True) * (1.0 / count)
    return (excess - scaled * mean) * scale


def pack_cols(hm33, ht33, hm32, hm31, hm22, ht22, hm21, ha2, hw2, hw3, left, right,
              m33, t33, m32, m31, m22, t22, m21, a2, w2, w3, st3, st2, flat, sems):
    rows, cols, ch = hm33.shape
    tall, wide, _ = hm22.shape
    moves = []
    for source, target in (
        (hm33.at[:, 0:8], m33.at[0]), (hm33.at[:, cols - 8 : cols], m33.at[1]),
        (ht33.at[:, 0:8], t33.at[0]), (ht33.at[:, cols - 8 : cols], t33.at[1]),
        (hm22.at[:, 0:8], m22.at[0]), (hm22.at[:, wide - 8 : wide], m22.at[1]),
        (ht22.at[:, 0:8], t22.at[0]), (ht22.at[:, wide - 8 : wide], t22.at[1]),
        (hm32.at[:, 0:8], m32.at[0]), (hm32.at[:, cols - 8 : cols], m32.at[1]),
        (hm31.at[:, 0:8], m31.at[0]), (hm31.at[:, cols - 8 : cols], m31.at[1]),
        (hm21.at[:, 0:8], m21.at[0]), (hm21.at[:, wide - 8 : wide], m21.at[1]),
        (ha2.at[:, 0:128], a2.at[0]), (ha2.at[:, (cols - 1) * 128 : cols * 128], a2.at[1]),
        (hw2, w2), (hw3, w3),
    ):
        moves.append(pltpu.make_async_copy(source, target, sems.at[len(moves)]))
        moves[-1].start()
    for move in moves[0:4] + moves[-2:]:
        move.wait()
    rest = moves[4:-2]
    for side, out in enumerate((left, right)):
        p = m33[side].reshape(rows * 8, ch)
        seeds = inject(p, t33[side].reshape(rows * 8, ch), w3[...])
        seeds = jnp.where(p.astype(F32) > 0, seeds, 0.0).reshape(rows, 8, ch)
        if side == 0:
            for move in rest:
                move.wait()
        for g, (base, width) in enumerate(((COL_SEED, 4), (COL_M32, 3), (COL_M31, 2))):
            pick = 8 - width if side else 0
            for h in range(2):
                lanes = slice(h * 128, (h + 1) * 128)
                own = (seeds[:, :, lanes], m32[side, :, :, lanes], m31[side, :, :, lanes])[g]
                stage = st3.at[(g * 2 + side) * 2 + h]
                stage[...] = own.astype(F32).reshape(rows * 8, 128)
                for c in range(width):
                    to = base + (c * 2 + h) * rows
                    flat[side, to : to + rows] = stage[pl.ds(pick + c, rows, stride=8), :]
        p = m22[side].reshape(tall * 8, 128)
        groups = (
            (COL_M22, 2, p.astype(F32)),
            (COL_I22, 2, inject(p, t22[side].reshape(tall * 8, 128), w2[...])),
            (COL_M21, 1, m21[side].astype(F32).reshape(tall * 8, 128)),
        )
        for g, (base, width, own) in enumerate(groups):
            pick = 8 - width if side else 0
            stage = st2.at[g * 2 + side]
            stage[...] = own
            for c in range(width):
                to = base + c * tall
                flat[side, to : to + tall] = stage[pl.ds(pick + c, tall, stride=8), :]
        flat[side, COL_A2 : COL_A2 + rows] = a2[side].astype(F32)
        out[...] = flat[side].astype(BF16)

def own_inject(m22, t22, m33, t33, w2, w3, k21, k22, i22, seeds, k21p, k22p):
    tall, wide, _ = m22.shape
    rows, cols, ch = m33.shape

    @pl.loop(0, tall // STEP2)
    def _(i):
        at = pl.ds(i * STEP2, STEP2)
        p = m22[at].reshape(STEP2 * wide, 128)
        i22[at] = inject(p, t22[at].reshape(STEP2 * wide, 128), w2[...]).reshape(STEP2, wide, 128)

    @pl.loop(0, rows // STEP3)
    def _(i):
        at = pl.ds(i * STEP3, STEP3)
        p = m33[at].reshape(STEP3 * cols, ch)
        value = inject(p, t33[at].reshape(STEP3 * cols, ch), w3[...])
        seeds[at] = jnp.where(p.astype(F32) > 0, value, 0.0).astype(BF16).reshape(STEP3, cols, ch)

    half = k21.shape[0] // 9
    span = k22.shape[1] // 3
    for dy in range(3):
        taps = [k21[(3 * dy + dx) * half : (3 * dy + dx + 1) * half].astype(F32) for dx in (0, 2, 1, 1)]
        rows_of = slice(dy * 128, (dy + 1) * 128)
        k21p[rows_of, 0:128] = jnp.concatenate(taps[:2], axis=0).T.astype(BF16)
        k21p[rows_of, 128:256] = jnp.concatenate(taps[2:], axis=0).T.astype(BF16)
        k22p[rows_of] = k22[:, dy * span : (dy + 1) * span]


def pack_rows(seeds, m32, m31, m22, i22, m21, a2, fl, fr, up, down, side_l, side_r, flat):
    rows, cols, _ = seeds.shape
    tall, wide, _ = m22.shape
    side_l[...] = fl[...].astype(F32)
    side_r[...] = fr[...].astype(F32)
    for side, out in enumerate((up, down)):
        for source, base, col_base, width in (
            (seeds, ROW_SEED, COL_SEED, 4), (m32, ROW_M32, COL_M32, 3), (m31, ROW_M31, COL_M31, 2),
        ):
            r0 = rows - width if side else 0
            for h in range(2):
                for k in range(width):
                    to = base + (k * 2 + h) * T3 + 4
                    flat[side, to : to + cols] = source[r0 + k, :, h * 128 : (h + 1) * 128].astype(F32)
                for c in range(width):
                    at = col_base + (c * 2 + h) * rows + r0
                    to = base + h * T3
                    flat.at[side][pl.ds(to + 4 - width + c, width, stride=2 * T3), :] = side_l[at : at + width]
                    flat.at[side][pl.ds(to + 4 + cols + c, width, stride=2 * T3), :] = side_r[at : at + width]
        for source, base, col_base, width in (
            (m22, ROW_M22, COL_M22, 2), (i22, ROW_I22, COL_I22, 2), (m21, ROW_M21, COL_M21, 1),
        ):
            r0 = tall - width if side else 0
            for k in range(width):
                to = base + k * T2 + 4
                flat[side, to : to + wide] = source[r0 + k].astype(F32)
                for c in range(width):
                    at = col_base + c * tall + r0 + k
                    flat[side, to - width + c : to - width + c + 1] = side_l[at : at + 1]
                    flat[side, to + wide + c : to + wide + c + 1] = side_r[at : at + 1]
        r0 = rows - 1 if side else 0
        line = a2[r0 : r0 + 1, :].astype(F32)
        to = ROW_A2 + 4
        for c in range(cols):
            flat[side, to + c : to + c + 1] = line[:, c * 128 : (c + 1) * 128]
        at = COL_A2 + r0
        flat[side, to - 1 : to] = side_l[at : at + 1]
        flat[side, to + cols : to + cols + 1] = side_r[at : at + 1]
        out[...] = flat[side].astype(BF16)


def conv(pick, kernel):
    span = kernel.shape[1] // 3
    total = None
    for dy in range(3):
        term = jnp.dot(pick(dy), kernel[:, dy * span : (dy + 1) * span], preferred_element_type=F32)
        total = term if total is None else total + term
    return shifted(total)


def shifted(total):
    n = total.shape[1] // 3
    before = pltpu.roll(total[:, :n], total.shape[0] - 1, 0)
    after = pltpu.roll(total[:, 2 * n :], 1, 0)
    return before + total[:, n : 2 * n] + after


def paired(x, kernel, row, count):
    size = count * x.shape[1]
    upper = x[pl.ds(row + 2, count)].reshape(size, 256)
    lower = x[pl.ds(row, count), :, 0:128].reshape(size, 128)
    return jnp.dot(upper, kernel[0:256], preferred_element_type=F32) + jnp.dot(
        lower, kernel[256:384], preferred_element_type=F32
    )


def doubled(total):
    size = total.shape[0]
    sides = total[:, 0:128]
    low = lax.broadcasted_iota(jnp.int32, sides.shape, 1) < 64
    sides = jnp.where(low, pltpu.roll(sides, size - 1, 0), pltpu.roll(sides, 1, 0))
    return total[:, 128:256] + sides + pltpu.roll(sides, 64, 1)


def store_pair(x, row, count, value):
    x[pl.ds(row, count), :, 0:128] = value
    x[pl.ds(row + 1, count), :, 128:256] = value


def block(x, row, count):
    def pick(dy):
        return x[pl.ds(row + 2 - dy, count)].reshape(count * x.shape[1], x.shape[2])

    return pick


def spread(part, where, u2, row):
    for a in range(2):
        for b in range(2):
            to = (2 * row + a) * WU + b
            u2[pl.ds(to, W3, stride=2), :] = jnp.where(where == 2.0 * a + b, part, 0.0)


def emit(a1, pieces, o1, result, sems):
    tiles = a1.shape[1] // 128
    group = GROUP

    moves = []
    for i in range(tiles // group):
        for part, (first, count, p1, out, top) in enumerate(pieces):
            high = lax.broadcasted_iota(jnp.int32, (count, 128), 1) >= 64
            shift = jnp.where(high, 1, 0)
            for j in range(group):
                t = i * group + j
                where = a1[first : first + count, t * 128 : (t + 1) * 128]
                turned = pltpu.roll(where, 64, 1)
                for odd in range(2):
                    own = (jnp.where(high, where, turned) if odd else jnp.where(high, turned, where)) - shift
                    value = p1[pl.ds(LEAD + 2 * t + odd, count, stride=WP), :]
                    slot = o1.at[(part * group + j) * 2 + odd]
                    for a in range(2):
                        slot[pl.ds(a, count, stride=2), :] = jnp.where(own == 2 * a, value, 0.0)
                    to = (2 * t + odd) * 128
                    out[:, to : to + 128] = slot[0 : 2 * count].astype(BF16)
            lanes = slice(2 * i * group * 128, 2 * (i + 1) * group * 128)
            moves.append(
                pltpu.make_async_copy(
                    out.at[:, lanes], result.at[top : top + 2 * count, lanes], sems.at[len(moves)]
                )
            )
            moves[-1].start()
    return moves


def steps(count, static):
    def run(body):
        if static:
            for i in range(count):
                body(i)
        else:
            pl.loop(0, count)(body)

    return run


def inner(seeds, m32, m31, m22, i22, m21, a2, a1, fl, fr, k33, k32, k31, k22, k21d,
          result, t33, t32, t31, ta, t22, ti, t21, y32, y31, y22, y21,
          e33, e32, e31, ea, e22, ei, e21, x33, x32, x31, u2, g22, g21, p1, o1, obuf, sem):
    rows, cols, _ = seeds.shape
    tall, wide, _ = m22.shape
    for source, stage, col_base, width in (
        (seeds, e33, COL_SEED, 4), (m32, e32, COL_M32, 3), (m31, e31, COL_M31, 2),
    ):

        @pl.loop(0, rows // 4)
        def _(i):
            for j in range(4):
                r = i * 4 + j
                to = pl.multiple_of(r * W3 + LEAD, 8)
                for h in range(2):
                    stage[h, pl.ds(to, cols)] = source[r, :, h * 128 : (h + 1) * 128].astype(F32)

        for h in range(2):
            for c in range(width):
                at = col_base + (c * 2 + h) * rows
                stage.at[h][pl.ds(LEAD - width + c, rows, stride=W3), :] = fl[at : at + rows].astype(F32)
                stage.at[h][pl.ds(LEAD + cols + c, rows, stride=W3), :] = fr[at : at + rows].astype(F32)
    for source, stage, col_base, width in (
        (m22, e22, COL_M22, 2), (i22, ei, COL_I22, 2), (m21, e21, COL_M21, 1),
    ):

        @pl.loop(0, tall // 4)
        def _(i):
            for j in range(4):
                r = i * 4 + j
                stage[pl.ds(pl.multiple_of(r * W2 + LEAD, 8), wide)] = source[r].astype(F32)

        for c in range(width):
            at = col_base + c * tall
            stage[pl.ds(LEAD - width + c, tall, stride=W2), :] = fl[at : at + tall].astype(F32)
            stage[pl.ds(LEAD + wide + c, tall, stride=W2), :] = fr[at : at + tall].astype(F32)
    for c in range(cols):
        ea[pl.ds(LEAD + c, rows, stride=W3), :] = a2[:, c * 128 : (c + 1) * 128].astype(F32)
    ea[pl.ds(LEAD - 1, rows, stride=W3), :] = fl[COL_A2 : COL_A2 + rows].astype(F32)
    ea[pl.ds(LEAD + cols, rows, stride=W3), :] = fr[COL_A2 : COL_A2 + rows].astype(F32)

    @steps(rows // 2, True)
    def _(i):
        for j in range(2):
            at = pl.ds(pl.multiple_of((i * 2 + j) * W3, W3), W3)
            for h in range(2):
                x33[i * 2 + j, :, h * 128 : (h + 1) * 128] = e33[h, at].astype(BF16)

    for x, kernel, stage, nxt, skip in ((x33, k33, e32, x32, 1), (x32, k32, e31, x31, 2)):
        count = nxt.shape[0] // SPLIT3

        @steps(SPLIT3, UNROLL[0])
        def _(i):
            row = i * count
            value = conv(block(x, row, count), kernel)
            at = pl.ds(pl.multiple_of((row + skip) * W3, W3), count * W3)
            for h in range(2):
                part = jnp.where(stage[h, at] > 0, value[:, h * 128 : (h + 1) * 128], 0.0)
                nxt[pl.ds(row, count), :, h * 128 : (h + 1) * 128] = part.astype(BF16).reshape(
                    count, W3, 128
                )

    count = (rows - 6) // SPLIT31

    @steps(SPLIT31, UNROLL[1])
    def _(i):
        row = i * count
        value = conv(block(x31, row, count), k31)
        for k in range(count):
            where = ea[pl.ds(pl.multiple_of((row + k + 3) * W3, W3), W3)]
            spread(value[k * W3 : (k + 1) * W3], where, u2, row + k)

    @steps((tall - 12) // 2, True)
    def _(i):
        for j in range(2):
            r = i * 2 + j
            at = pl.ds(pl.multiple_of((r + 6) * W2, W2), W2)
            arriving = u2[pl.ds(pl.multiple_of(r * WU + LEAD, 8), W2)] + ei[at]
            store_pair(g22, r, 1, jnp.where(e22[at] > 0, arriving, 0.0).astype(BF16).reshape(1, W2, 128))

    count = (tall - 14) // SPLIT2

    @steps(SPLIT2, UNROLL[2])
    def _(i):
        row = i * count
        value = shifted(paired(g22, k22, row, count))
        at = pl.ds(pl.multiple_of((row + 7) * W2, W2), count * W2)
        value = jnp.where(e21[at] > 0, value, 0.0)
        store_pair(g21, row, count, value.astype(BF16).reshape(count, W2, 128))

    half = (tall - 16) // SPLIT2

    @steps(SPLIT2, UNROLL[3])
    def _(i):
        row = i * half
        value = doubled(paired(g21, k21d, row, half))
        for k in range(half):
            p1[pl.ds(pl.multiple_of((row + k) * WP, 8), W2)] = value[k * W2 : (k + 1) * W2]

    moves = emit(a1, ((8, tall - 16, p1, obuf, 16),), o1, result, sem)
    for side in range(2):
        for target, stage, count, width in (
            (t33, e33, 2, W3), (t32, e32, 1, W3), (t31, e31, 2, W3),
        ):
            r0 = (rows - count) * side
            target[side] = stage[:, r0 * width : (r0 + count) * width]
        for target, stage, count, width, total in (
            (ta, ea, 3, W3, rows), (t22, e22, 6, W2, tall), (ti, ei, 6, W2, tall), (t21, e21, 7, W2, tall),
        ):
            r0 = (total - count) * side
            target[side] = stage[r0 * width : (r0 + count) * width]
        for target, source, count in (
            (y32, x32, rows - 2), (y31, x31, rows - 4), (y22, g22, tall - 12), (y21, g21, tall - 14),
        ):
            r0 = (count - 2) * side
            target[side] = source[r0 : r0 + 2, :, 0 : target.shape[3]]
    for move in moves:
        move.wait()


def outer(t33, t32, t31, ta, t22, ti, t21, y32, y31, y22, y21, above, below, a1,
          k33, k32, k31, k22, k21d, partial, result,
          halo, e33, e32, e31, ea, e22, ei, e21, x33, x32, x31, u2, g22, g21, p1, o1, obuf, sem):
    del partial
    tall = result.shape[0] // 2
    halo[0] = above[...].astype(F32)
    halo[1] = below[...].astype(F32)
    for side in range(2):
        for own, stage, base, width in (
            (t33, e33, ROW_SEED, 4), (t32, e32, ROW_M32, 3), (t31, e31, ROW_M31, 2),
        ):
            keep = own.shape[2]
            for h in range(2):
                to = 0 if side else width * W3
                stage[side, h, to : to + keep] = own[side, h]
                for k in range(width):
                    at = base + (k * 2 + h) * T3
                    to = k * W3 + 4 + (keep if side else 0)
                    stage[side, h, to : to + T3] = halo[side, at : at + T3]
        for own, stage, base, width, narrow, full in (
            (ta, ea, ROW_A2, 1, T3, W3), (t22, e22, ROW_M22, 2, T2, W2),
            (ti, ei, ROW_I22, 2, T2, W2), (t21, e21, ROW_M21, 1, T2, W2),
        ):
            keep = own.shape[1]
            to = 0 if side else width * full
            stage[side, to : to + keep] = own[side]
            for k in range(width):
                at = base + k * narrow
                to = k * full + 4 + (keep if side else 0)
                stage[side, to : to + narrow] = halo[side, at : at + narrow]
        for r in range(6):
            for h in range(2):
                x33[side, r, :, h * 128 : (h + 1) * 128] = e33[side, h, r * W3 : (r + 1) * W3].astype(BF16)
        fresh, kept = (2, 0) if side else (0, 4)
        x32[side, kept : kept + 2] = y32[side]
        x31[side, kept : kept + 2] = y31[side]
        fresh, kept = (2, 0) if side else (0, 8)
        store_pair(g22.at[side], kept, 2, y22[side])
        store_pair(g21.at[side], kept, 2, y21[side])

    for x, kernel, stage, nxt in ((x33, k33, e32, x32), (x32, k32, e31, x31)):
        for side in range(2):
            value = conv(block(x.at[side], 0, 4), kernel)
            for h in range(2):
                part = value[:, h * 128 : (h + 1) * 128]
                part = jnp.where(stage[side, h] > 0, part, 0.0).astype(BF16).reshape(4, W3, 128)
                nxt[side, 2 * side : 2 * side + 4, :, h * 128 : (h + 1) * 128] = part
    for side in range(2):
        value = conv(block(x31.at[side], 0, 4), k31)
        for k in range(4):
            spread(value[k * W3 : (k + 1) * W3], ea[side, k * W3 : (k + 1) * W3], u2.at[side], k)
        for r in range(8):
            at = slice(r * W2, (r + 1) * W2)
            arriving = u2[side, r * WU + LEAD : r * WU + LEAD + W2] + ei[side, at]
            arriving = jnp.where(e22[side, at] > 0, arriving, 0.0).astype(BF16)
            store_pair(g22.at[side], 2 * side + r, 1, arriving.reshape(1, W2, 128))

    def second(side):
        value = shifted(paired(g22.at[side], k22, 0, 8))
        value = jnp.where(e21[side] > 0, value, 0.0).astype(BF16)
        store_pair(g21.at[side], 2 * side, 8, value.reshape(8, W2, 128))

    def first(side):
        value = doubled(paired(g21.at[side], k21d, 0, 8))
        for k in range(8):
            p1[side, k * WP : k * WP + W2] = value[k * W2 : (k + 1) * W2]

    for step in (second, first):
        if SIDES == 1:
            pl.loop(0, 2)(step)
        else:
            for side in range(2):
                step(side)

    moves = emit(
        a1,
        ((0, 8, p1.at[0], obuf.at[0], 0), (tall - 8, 8, p1.at[1], obuf.at[1], 2 * tall - 16)),
        o1, result, sem,
    )
    for move in moves:
        move.wait()


def whole(array):
    zeros = (0,) * len(array.shape)
    return pl.BlockSpec(array.shape, lambda i: zeros)


STORED = pl.BlockSpec(memory_space=pltpu.MemorySpace.HBM)


def call(body, args, outs, scratch=(), specs=None, out_specs=None, aliases=None, cost=0, limit=8, flags=None):
    shapes = [jax.ShapeDtypeStruct(s, d) for s, d in outs]
    return pl.pallas_call(
        body,
        grid=(1,),
        in_specs=specs or [whole(a) for a in args],
        out_specs=out_specs or [whole(s) for s in shapes],
        out_shape=shapes,
        input_output_aliases=aliases or {},
        scratch_shapes=[pltpu.VMEM(*s) if isinstance(s, tuple) else s for s in scratch],
        cost_estimate=pl.CostEstimate(flops=cost, bytes_accessed=4000000, transcendentals=0),
        compiler_params=pltpu.CompilerParams(vmem_limit_bytes=limit << 20, flags=flags),
    )(*args)


def swap(first, last, axis):
    count = lax.axis_size(axis)
    from_before = lax.ppermute(last, axis, [(i, i + 1) for i in range(count - 1)])
    from_after = lax.ppermute(first, axis, [(i + 1, i) for i in range(count - 1)])
    return from_before, from_after


def shards(m21, m22, m31, m32, m33, t22, t33, a1, a2, w2, w3, k21, k22, k31, k32, k33):
    rows, cols, ch3 = m33.shape
    tall, wide, ch2 = m22.shape
    w2 = w2.reshape(1, ch2)
    w3 = w3.reshape(1, ch3)
    args = tuple(
        pltpu.with_memory_space_constraint(x, pltpu.MemorySpace.HBM)
        for x in (m33, t33, m32, m31, m22, t22, m21, a2, w2, w3)
    )
    left, right = call(
        pack_cols, args,
        [((COL_TOTAL, 128), BF16), ((COL_TOTAL, 128), BF16)],
        scratch=[
            ((2, rows, 8, ch3), BF16), ((2, rows, 8, ch3), BF16), ((2, rows, 8, ch3), BF16),
            ((2, rows, 8, ch3), BF16), ((2, tall, 8, ch2), BF16), ((2, tall, 8, ch2), BF16),
            ((2, tall, 8, ch2), BF16), ((2, rows, 128), a2.dtype), (w2.shape, F32), (w3.shape, F32),
            ((12, rows * 8, 128), F32), ((6, tall * 8, 128), F32), ((2, COL_TOTAL, 128), F32),
            pltpu.SemaphoreType.DMA((18,)),
        ],
        specs=[STORED] * 10, cost=10**9, limit=LIM[0], flags=FLAGS[0],
    )
    fl, fr = swap(left, right, "col")
    i22, seeds, k21d, k22 = call(
        own_inject, (m22, t22, m33, t33, w2, w3, k21.T, k22),
        [((tall, wide, ch2), F32), ((rows, cols, ch3), BF16), ((3 * ch2, 256), BF16), ((3 * ch2, 384), BF16)],
        cost=10**9, limit=LIM[1], flags=FLAGS[1],
    )
    up, down = call(
        pack_rows, (seeds, m32, m31, m22, i22, m21, a2, fl, fr),
        [((ROW_TOTAL, 128), BF16), ((ROW_TOTAL, 128), BF16)],
        scratch=[((COL_TOTAL, 128), F32), ((COL_TOTAL, 128), F32), ((2, ROW_TOTAL, 128), F32)],
        cost=10**9, limit=LIM[2], flags=FLAGS[2],
    )
    above, below = swap(up, down, "row")
    area3, area2 = rows * W3, tall * W2
    edges = [
        ((2, 2, 2 * W3, 128), F32), ((2, 2, W3, 128), F32), ((2, 2, 2 * W3, 128), F32), ((2, 3 * W3, 128), F32),
        ((2, 6 * W2, 128), F32), ((2, 6 * W2, 128), F32), ((2, 7 * W2, 128), F32),
        ((2, 2, W3, ch3), BF16), ((2, 2, W3, ch3), BF16), ((2, 2, W2, ch2), BF16), ((2, 2, W2, ch2), BF16),
    ]
    shape = (2 * tall, 2 * wide * 64)
    partial, *state = call(
        inner,
        (seeds, m32, m31, m22, i22, m21, a2, a1, fl, fr, k33, k32, k31, k22, k21d),
        [(shape, BF16)] + edges,
        out_specs=[STORED] + [whole(jax.ShapeDtypeStruct(s, d)) for s, d in edges],
        scratch=[
            ((2, area3, 128), F32), ((2, area3, 128), F32), ((2, area3, 128), F32), ((area3, 128), F32),
            ((area2, 128), F32), ((area2, 128), F32), ((area2, 128), F32),
            ((rows, W3, ch3), BF16), ((rows - 2, W3, ch3), BF16), ((rows - 4, W3, ch3), BF16),
            (((tall - 12) * WU, 128), F32), ((tall - 11, W2, 256), BF16), ((tall - 13, W2, 256), BF16),
            (((tall - 16) * WP, 128), F32), ((2 * GROUP, 2 * tall - 32, 128), F32), ((2 * tall - 32, shape[1]), BF16),
            pltpu.SemaphoreType.DMA((wide // 2 // GROUP,)),
        ],
        cost=10**10, limit=LIM[3], flags=FLAGS[3],
    )
    args = (*state, above, below, a1, k33, k32, k31, k22, k21d)
    (result,) = call(
        outer, (*args, partial), [(shape, BF16)],
        specs=[whole(a) for a in args] + [STORED], out_specs=[STORED], aliases={len(args): 0},
        scratch=[
            ((2, ROW_TOTAL, 128), F32),
            ((2, 2, 6 * W3, 128), F32), ((2, 2, 4 * W3, 128), F32), ((2, 2, 4 * W3, 128), F32),
            ((2, 4 * W3, 128), F32), ((2, 8 * W2, 128), F32), ((2, 8 * W2, 128), F32), ((2, 8 * W2, 128), F32),
            ((2, 6, W3, ch3), BF16), ((2, 6, W3, ch3), BF16), ((2, 6, W3, ch3), BF16),
            ((2, 8 * WU, 128), F32), ((2, 11, W2, 256), BF16), ((2, 11, W2, 256), BF16),
            ((2, 8 * WP, 128), F32), ((4 * GROUP, 16, 128), F32), ((2, 16, shape[1]), BF16),
            pltpu.SemaphoreType.DMA((2 * (wide // 2 // GROUP),)),
        ],
        cost=10**9, limit=LIM[4], flags=FLAGS[4],
    )
    return result


def solution(mesh):
    in_specs = (P("row", "col", None),) * 7 + (P("row", "col"),) * 2 + (P(),) * 7
    return jax.shard_map(
        shards, mesh=mesh, in_specs=in_specs, out_specs=P("row", "col"), check_vma=False
    )
```
